32 devices in a mesh: beam: 2 (over y), tm: 4 (over x, core), dm: 4 (over z).
Axes of the slice: x: 2, y: 2, z: 4, core: 2. Of those that a mesh axis runs over, the one named last changes fastest.
Arguments:
- series: float32 [16, 524288], P(('beam', 'dm'), 'tm'), parts along dimension 0, may hold values from -16 to 16
- cand_start: int32 [8, 4, 4, 16], P(('beam', 'tm'), 'dm'), parts along dimension 0, may hold values from 0 to 8064
- cand_count: int32 [8, 4, 4], P(('beam', 'tm'), 'dm'), parts along dimension 0, may hold values from 0 to 16, as said below
Outputs:
- harmonic_sum: float32 [16, 32768], P(('beam', 'dm'), 'tm'), parts along dimension 0
- sifted: float32 [8, 4, 4, 16, 128], P(('beam', 'tm'), 'dm'), parts along dimension 0
The draws below stay inside these ranges and needn't reach their ends.
There are 2 independent parts, one for each index of `beam`. The reference program is written for one: setup_inputs(seed, part) draws one part's arguments, and reference() takes and returns one part's arrays. A program takes and returns all parts, laid end to end along the dimension named above; each array names one. Nothing has to cross between parts.
Inputs may be any that keep to these rules, and one draw needn't show every extreme that they name: `cand_count`: in every draw some destination band receives 16 live slots from every source band and frequency shard.
All inputs are finite; a program needn't handle non-finite values.
Results may differ from the reference program's by a relative error of at most 0.00015.
Values sent between devices are 32-bit elements; how exact they have to be, the bound alone decides.
A program may use at most 128 MiB of HBM per device.

```python
import jax
import jax.numpy as jnp
from jax import lax

DM_DEV = 2
NT = 524288
N1 = 512
HARM = 8
BW = 128
CAP = 16
NDM = 8
TSHARDS = 4
BANDS = 4
NH = 32768
FL = 8192


def draw_series(key, part):
    noise_key, echo_key, gain_key = jax.random.split(jax.random.fold_in(key, 11), 3)
    echo_lag = NT // N1
    noise = jax.random.truncated_normal(noise_key, -4.0, 4.0, (NDM, NT + echo_lag), jnp.float32)
    echo_level = jax.random.uniform(echo_key, (NDM, 1), jnp.float32, 0.4, 0.8)
    time_ramp = jnp.ones((1, NT), jnp.float32)
    row_gain = jax.random.uniform(gain_key, (NDM, 1), jnp.float32, 0.5, 2.0)
    return (row_gain * time_ramp * (noise[:, echo_lag:] + echo_level * noise[:, :NT])).astype(jnp.float32)


def draw_cand_count(key, part):
    base_key, light_key, chosen_key = jax.random.split(jax.random.fold_in(key, 23), 3)
    counts = jax.random.randint(base_key, (TSHARDS, BANDS, BANDS), 0, CAP + 1)
    lighter = jax.random.randint(light_key, (BANDS,), 0, 2)
    chosen = jax.random.randint(chosen_key, (), 0, BANDS)
    targets = jnp.arange(BANDS, dtype=jnp.int32)
    counts = jnp.where(lighter[None, None, :] == 1, counts // 2, counts)
    counts = jnp.where(targets[None, None, :] == chosen, CAP, counts)
    return counts.astype(jnp.int32)


def place_ends(result, key, least, top_value):
    extent = result.shape
    index_at = [jax.random.randint(jax.random.fold_in(key, axis), (), 0, extent[axis]) for axis in range(len(extent))]
    result = result.at[tuple(index_at)].set(least)
    longest = extent.index(max(extent))
    index_at[longest] = (index_at[longest] + 1) % extent[longest]
    return result.at[tuple(index_at)].set(top_value)


def setup_inputs(seed: int = 0, part: int = 0) -> dict:
    key_of = jax.random.split(jax.random.key(seed), 4)
    own_keys = jax.random.split(jax.random.fold_in(key_of[3], part), 4)
    return {
        "series": draw_series(jax.random.fold_in(jax.random.fold_in(key_of[3], part), 71), part),
        "cand_start": place_ends(jax.random.randint(own_keys[1], (TSHARDS, BANDS, BANDS, CAP), 0, FL - BW + 1), jax.random.fold_in(own_keys[1], 1), 0, FL - BW).astype(jnp.int32),
        "cand_count": draw_cand_count(jax.random.fold_in(jax.random.fold_in(key_of[3], part), 71), part),
    }


EPSILON = 1e-06

def reference(series, cand_start, cand_count):
    spectrum = jnp.fft.rfft(series, axis=-1)[:, :NT // 2]
    power_bins = ((jnp.real(spectrum) ** 2 + jnp.imag(spectrum) ** 2) / NT).astype(jnp.float32)
    row_mean = lax.optimization_barrier(jnp.mean(power_bins, axis=1, keepdims=True))
    deviation = power_bins - row_mean
    spread = lax.optimization_barrier(jnp.mean(deviation * deviation, axis=1, keepdims=True))
    scores = deviation / jnp.sqrt(spread + EPSILON)
    summed = scores[:, :NH]
    for harmonic in range(2, HARM + 1):
        summed = summed + scores[:, 0:harmonic * NH:harmonic]
    banded = summed.reshape(BANDS, DM_DEV, TSHARDS, FL)
    peak_rows = lax.optimization_barrier(jnp.max(banded, axis=1))
    band_level = lax.optimization_barrier(jnp.sum(banded, axis=1)) / DM_DEV
    bin_span = cand_start[..., None] + jnp.arange(BW, dtype=jnp.int32)
    shard_ids = jnp.arange(TSHARDS, dtype=jnp.int32)[:, None, None, None, None]
    source_ids = jnp.arange(BANDS, dtype=jnp.int32)[None, :, None, None, None]
    target_ids = jnp.arange(BANDS, dtype=jnp.int32)[None, None, :, None, None]
    top_values = peak_rows[source_ids, shard_ids, bin_span]
    low_values = band_level[target_ids, shard_ids, bin_span]
    slot_ids = jnp.arange(CAP, dtype=jnp.int32)[None, None, None, :, None]
    live_slots = slot_ids < cand_count[..., None, None]
    sifted = jnp.where(live_slots, top_values - low_values, jnp.float32(0.0))
    sifted = jnp.transpose(sifted, (0, 2, 1, 3, 4))
    return (summed, sifted)
```

```python
import math

import jax
import jax.numpy as jnp
import numpy as np
from jax import lax
from jax.experimental import pallas as pl
from jax.experimental.pallas import tpu as pltpu
from jax.sharding import PartitionSpec as P

NT = 524288
N1 = 512
HARM = 8
BW = 128


EPSILON = 1e-06


def contract(pattern, left, right):
    return jnp.einsum(pattern, left, right, precision=lax.Precision.HIGHEST)


def phase_table(left, right, period):
    turns = left[:, None] * right[None, :] % period
    angle = turns.astype(jnp.float32) * (2.0 * math.pi / period)
    return (jnp.cos(angle), jnp.sin(angle))


def twist(real_part, imag_part, cos_twist, sin_twist):
    return (
        real_part * cos_twist + imag_part * sin_twist,
        imag_part * cos_twist - real_part * sin_twist,
    )


def locate_column(column, per_shard):
    return (column // per_shard, column % per_shard)


def harmonic_tables(column_count, shards, per_shard, harmonics):
    listing = [[[] for harmonic in range(harmonics)] for holder in range(shards)]
    for harmonic in range(1, harmonics + 1):
        for residue in range(column_count):
            product = harmonic * residue
            holder, position = locate_column(product % column_count, per_shard)
            listing[holder][harmonic - 1].append((residue, position, product // column_count))
    slot_width = max((max((len(entries) for entries in group)) for group in listing))
    residue_tab = np.zeros((shards, harmonics, slot_width), np.int32)
    position_tab = np.zeros((shards, harmonics, slot_width), np.int32)
    base_tab = np.zeros((shards, harmonics, slot_width), np.int32)
    valid_tab = np.zeros((shards, harmonics, slot_width), np.float32)
    for holder in range(shards):
        for index in range(harmonics):
            for slot, entry in enumerate(listing[holder][index]):
                residue_tab[holder, index, slot] = entry[0]
                position_tab[holder, index, slot] = entry[1]
                base_tab[holder, index, slot] = entry[2]
                valid_tab[holder, index, slot] = 1.0
    return (residue_tab, position_tab, base_tab, valid_tab)


def per_device(series, cand_start, cand_count):
    dm_rows, samples_dev = series.shape
    shards = lax.axis_size("tm")
    my_index = lax.axis_index("tm")
    inner_len = NT // N1
    kept_bins = inner_len // 2
    per_shard = N1 // shards
    columns = jnp.arange(N1, dtype=jnp.int32)
    coarse_rows = samples_dev // inner_len
    rows_local = series.reshape(dm_rows, coarse_rows, inner_len)
    cos_first, sin_first = phase_table(columns, columns, N1)
    narrow = inner_len // shards
    inner_ids = my_index * narrow + jnp.arange(narrow, dtype=jnp.int32)
    cos_twist, sin_twist = phase_table(inner_ids, columns, NT)
    samples = lax.all_to_all(rows_local, "tm", split_axis=2, concat_axis=1, tiled=True)
    real_part = contract("nab,ar->nbr", samples, cos_first)
    imag_part = -contract("nab,ar->nbr", samples, sin_first)
    twist_re, twist_im = twist(real_part, imag_part, cos_twist, sin_twist)
    cos_second, sin_second = phase_table(
        jnp.arange(inner_len, dtype=jnp.int32), jnp.arange(kept_bins, dtype=jnp.int32), inner_len
    )
    part_re = lax.all_to_all(twist_re, "tm", split_axis=2, concat_axis=1, tiled=True)
    part_im = lax.all_to_all(twist_im, "tm", split_axis=2, concat_axis=1, tiled=True)
    x_re = contract("nbr,bk->nrk", part_re, cos_second) + contract(
        "nbr,bk->nrk", part_im, sin_second
    )
    x_im = contract("nbr,bk->nrk", part_im, cos_second) - contract(
        "nbr,bk->nrk", part_re, sin_second
    )
    power_bins = (x_re * x_re + x_im * x_im) / NT
    bin_total = NT // 2
    row_mean = lax.psum(jnp.sum(power_bins, axis=(1, 2)), "tm") / bin_total
    centered = power_bins - row_mean[:, None, None]
    spread = lax.psum(jnp.sum(centered * centered, axis=(1, 2)), "tm") / bin_total
    scores = centered / jnp.sqrt(spread + EPSILON)[:, None, None]
    score_flat = scores.reshape(dm_rows, per_shard * kept_bins)
    cycles = NT // (2 * HARM) // N1
    residue_tab, position_tab, base_tab, valid_tab = harmonic_tables(N1, shards, per_shard, HARM)
    my_positions = jnp.asarray(position_tab)[my_index]
    my_bases = jnp.asarray(base_tab)[my_index]
    my_valid = jnp.asarray(valid_tab)[my_index]
    cycle_ids = jnp.arange(cycles, dtype=jnp.int32)
    picked_parts = []
    for harmonic in range(1, HARM + 1):
        flat_index = (
            my_positions[harmonic - 1][:, None] * kept_bins
            + my_bases[harmonic - 1][:, None]
            + harmonic * cycle_ids[None, :]
        )
        values = jnp.take(score_flat, flat_index.reshape(-1), axis=1).reshape(dm_rows, -1, cycles)
        picked_parts.append(values * my_valid[harmonic - 1][None, :, None])
    picked = jnp.stack(picked_parts, axis=1)
    my_residues = jnp.asarray(residue_tab)[my_index].reshape(-1)
    spread_values = jnp.swapaxes(picked.reshape(dm_rows, -1, cycles), 1, 2)
    dense = jnp.zeros((dm_rows, cycles, N1), jnp.float32).at[:, :, my_residues].add(spread_values)
    dense = dense.reshape(dm_rows, cycles * N1)
    summed = lax.psum_scatter(dense.T, "tm", scatter_dimension=0, tiled=True)
    harmonic_sum = summed.T
    slot_total = cand_start.shape[3]
    offsets = jnp.arange(BW, dtype=jnp.int32)
    starts = cand_start[0, 0]
    counts = cand_count[0, 0]
    live_slots = jnp.arange(slot_total, dtype=jnp.int32)[None, :] < counts[:, None]
    markers = jnp.where(live_slots, starts, -1).astype(jnp.float32)
    bin_spans = starts[..., None] + offsets
    band_level = jnp.sum(harmonic_sum, axis=0) / dm_rows
    gathered = jnp.take(harmonic_sum, bin_spans, axis=1)
    blocks = jnp.moveaxis(gathered, 0, 2)
    blocks_in = lax.all_to_all(blocks, "dm", split_axis=0, concat_axis=0, tiled=True)
    markers_in = lax.all_to_all(markers, "dm", split_axis=0, concat_axis=0, tiled=True)
    chosen = markers_in.astype(jnp.int32)
    level = jnp.take(band_level, jnp.maximum(chosen, 0)[..., None] + offsets, axis=0)
    sifted = jnp.where(chosen[..., None] >= 0, jnp.max(blocks_in, axis=2) - level, 0.0)
    return (harmonic_sum, sifted[None, None])


MESH = pl.DeviceIdType.MESH
LANES = 128
CHUNKS = 4
VMEM_LIMIT = 60 * 1024 * 1024


def split_pair(value):
    high = value.astype(jnp.bfloat16)
    return high, (value - high.astype(jnp.float32)).astype(jnp.bfloat16)


def host_split(table):
    high = table.astype(jnp.bfloat16)
    low = (table - high.astype(np.float64)).astype(jnp.bfloat16)
    return high, low


def dft_tables(shards, cores):
    inner = NT // N1
    kept = inner // 2
    coarse = N1 // shards
    res = N1 // cores
    ids = np.arange(N1)
    turn = 2.0 * np.pi * (np.outer(ids, ids) % N1) / N1
    first = np.empty((cores, shards, 2 * res, 3 * coarse), jnp.bfloat16)
    for core in range(cores):
        for shard in range(shards):
            part = turn[core * res : (core + 1) * res, shard * coarse : (shard + 1) * coarse]
            high, low = host_split(np.concatenate([np.cos(part), -np.sin(part)], axis=0))
            first[core, shard] = np.concatenate([high, high, low], axis=1)
    turn = 2.0 * np.pi * np.outer(ids, np.arange(inner)) / NT
    twist_tab = np.stack([np.cos(turn), np.sin(turn)], axis=0).astype(np.float32)
    twist_tab = twist_tab.reshape(2, cores, res, inner).transpose(1, 0, 2, 3)
    turn = 2.0 * np.pi * (np.outer(np.arange(kept), np.arange(inner)) % inner) / inner
    second = np.stack(host_split(np.cos(turn)) + host_split(np.sin(turn)), axis=0)
    return first, twist_tab, second


def spectrum_kernel(
    x_ref, first_hbm, twist_hbm, second_hbm, out_ref,
    gathered, outgoing, x_tab, first, twist_tab, second, partial, b_high, b_low, power, picks, select,
    load_sem, send_sem, recv_sem,
):
    me = lax.axis_index("tm")
    core, chip = lax.rem(me, 2), me // 2
    sibling = me + 1 - 2 * core
    across = lax.rem(me + 2, 4)
    diagonal = lax.rem(sibling + 2, 4)
    size = gathered.shape[1]
    step = size // CHUNKS
    shards, inner = gathered.shape[0], partial.shape[1]
    coarse = size // (inner // LANES)
    res = partial.shape[0] // 2
    kept = power.shape[1]

    loads = [
        pltpu.make_async_copy(first_hbm.at[core], first, load_sem.at[0]),
        pltpu.make_async_copy(twist_hbm.at[core], twist_tab, load_sem.at[1]),
        pltpu.make_async_copy(second_hbm, second, load_sem.at[2]),
    ]
    for load in loads:
        load.start()
    barrier = pltpu.get_barrier_semaphore()
    for peer in (sibling, across):
        pl.semaphore_signal(barrier, inc=1, device_id={"tm": peer}, device_id_type=MESH)
    for piece in range(CHUNKS):
        row_a = x_ref[pl.ds(2 * piece * step, step, stride=2), :]
        row_b = x_ref[pl.ds(2 * piece * step + 1, step, stride=2), :]
        outgoing[piece * step : (piece + 1) * step, :] = jnp.where(chip == 0, row_b, row_a)
        gathered[me, piece * step : (piece + 1) * step, :] = jnp.where(chip == 0, row_a, row_b)
    pl.semaphore_wait(barrier, 2)

    def remote(src, dst, index, peer):
        return pltpu.make_async_remote_copy(
            src_ref=src, dst_ref=dst, send_sem=send_sem.at[index], recv_sem=recv_sem.at[index],
            device_id={"tm": peer}, device_id_type=MESH,
        )

    crossing = []
    for piece in range(CHUNKS):
        rows = pl.ds(piece * step, step)
        crossing.append(remote(outgoing.at[rows], gathered.at[me, rows], 1 + piece, across))
        crossing[-1].start()
    own = remote(gathered.at[me], gathered.at[me], 0, sibling)
    own.start()

    lane_ids = lax.broadcasted_iota(jnp.int32, (res, N1), 1)
    res_ids = lax.broadcasted_iota(jnp.int32, (res, N1), 0) + core * res
    slot = 0
    for harmonic in range(1, HARM + 1):
        target = lane_ids * harmonic - res_ids
        for cycle in range(harmonic):
            hit = jnp.where(target == cycle * N1, 1.0, 0.0)
            select[slot * res : (slot + 1) * res, :] = hit.astype(jnp.bfloat16)
            slot += 1
    for load in loads:
        load.wait()

    def accumulate(shard, fresh):
        for group in range(inner // LANES):
            high, low = split_pair(gathered[shard, pl.ds(group, coarse, stride=inner // LANES), :])
            cols = slice(group * LANES, (group + 1) * LANES)
            x_tab[0:coarse, cols] = high
            x_tab[coarse : 2 * coarse, cols] = low
            x_tab[2 * coarse : 3 * coarse, cols] = high
        for block in range(inner // 256):
            cols = slice(block * 256, (block + 1) * 256)
            term = jnp.dot(first[shard], x_tab[:, cols], preferred_element_type=jnp.float32)
            partial[:, cols] = term if fresh else partial[:, cols] + term

    accumulate(me, True)
    own.wait_recv()
    accumulate(sibling, False)
    forwards = []
    for piece in range(CHUNKS):
        rows = pl.ds(piece * step, step)
        crossing[piece].wait_recv()
        forwards.append(remote(gathered.at[across, rows], gathered.at[across, rows], 1 + CHUNKS + piece, sibling))
        forwards[-1].start()
    accumulate(across, False)
    for forward in forwards:
        forward.wait_recv()
    accumulate(diagonal, False)

    for block in range(inner // 256):
        cols = slice(block * 256, (block + 1) * 256)
        real_part, imag_part = twist(
            partial[0:res, cols], partial[res : 2 * res, cols], twist_tab[0, :, cols], twist_tab[1, :, cols]
        )
        b_high[0:res, cols], b_low[0:res, cols] = split_pair(real_part)
        b_high[res : 2 * res, cols], b_low[res : 2 * res, cols] = split_pair(imag_part)

    def against(table, right):
        return lax.dot_general(table, right, (((1,), (1,)), ((), ())), preferred_element_type=jnp.float32)

    half = kept // 2

    @pl.loop(0, 2)
    def _(part):
        rows = pl.ds(pl.multiple_of(part * half, half), half)
        by_cos = against(second[0, rows], b_high[...]) + against(second[0, rows], b_low[...])
        by_cos = by_cos + against(second[1, rows], b_high[...])
        by_sin = against(second[2, rows], b_high[...]) + against(second[2, rows], b_low[...])
        by_sin = by_sin + against(second[3, rows], b_high[...])
        x_re = by_cos[:, 0:res] + by_sin[:, res:]
        x_im = by_cos[:, res:] - by_sin[:, 0:res]
        bins = (x_re * x_re + x_im * x_im) / NT
        for column in range(res // LANES):
            power[column, rows, :] = bins[:, column * LANES : (column + 1) * LANES]

    total = jnp.sum(power[...])
    mean = total / (kept * res)
    off = power[...] - mean
    deviation = jnp.sum(off * off)

    cycles = NT // (2 * HARM) // N1
    slot = 0
    for harmonic in range(1, HARM + 1):
        for cycle in range(harmonic):
            for column in range(res // LANES):
                high, low = split_pair(power[column, pl.ds(cycle, cycles, stride=harmonic), :])
                cols = slice(slot * res + column * LANES, slot * res + (column + 1) * LANES)
                picks[0:cycles, cols] = high
                picks[cycles : 2 * cycles, cols] = low
            slot += 1
    sums = jnp.dot(picks[...], select[...], preferred_element_type=jnp.float32)
    sums = sums[0:cycles] + sums[cycles : 2 * cycles]
    each = cycles // shards
    lead = N1 // LANES
    for shard in range(shards):
        for column in range(lead):
            out_ref[shard, column * each : (column + 1) * each, :] = sums[
                shard * each : (shard + 1) * each, column * LANES : (column + 1) * LANES
            ]
        out_ref[shard, lead * each : lead * each + 8, :] = jnp.full((8, LANES), mean, jnp.float32)
        out_ref[shard, lead * each + 8 : lead * each + 16, :] = jnp.full((8, LANES), deviation, jnp.float32)
    own.wait_send()
    for copy in crossing + forwards:
        copy.wait_send()


def exchange_kernel(
    part_ref, mark_ref, harm_ref, level_ref, peaks_ref, marks_ref,
    parts, marks, peaks, top, send_sem, recv_sem,
):
    me, band = lax.axis_index("tm"), lax.axis_index("dm")
    shards, bands = lax.axis_size("tm"), lax.axis_size("dm")
    lead = N1 // LANES
    each = (part_ref.shape[1] - 16) // lead

    barrier = pltpu.get_barrier_semaphore()
    for axis, count, here in (("tm", shards, me), ("dm", bands, band)):
        for away in range(1, count):
            peer = lax.rem(here + away, count)
            pl.semaphore_signal(barrier, inc=1, device_id={axis: peer}, device_id_type=MESH)
    pl.semaphore_wait(barrier, shards + bands - 2)

    def remote(src, dst, index, axis, peer):
        return pltpu.make_async_remote_copy(
            src_ref=src, dst_ref=dst, send_sem=send_sem.at[index], recv_sem=recv_sem.at[index],
            device_id={axis: peer}, device_id_type=MESH,
        )

    first_hop, second_hop, third_hop = [], [], []
    for away in range(1, shards):
        peer = lax.rem(me + away, shards)
        first_hop.append(remote(part_ref.at[peer], parts.at[me], away - 1, "tm", peer))
        first_hop[-1].start()
    for away in range(1, bands):
        peer = lax.rem(band + away, bands)
        second_hop.append(remote(mark_ref.at[peer], marks.at[band], shards + away, "dm", peer))
        second_hop[-1].start()
    for copy in first_hop:
        copy.wait_recv()
    parts[me] = part_ref[me]

    bin_total = NT // 2
    share = bin_total // 2
    rows = []
    for row in range(2):
        left, right = parts[2 * row], parts[2 * row + 1]
        base = lead * each
        mean_l, mean_r = left[base : base + 8], right[base : base + 8]
        row_mean = 0.5 * (mean_l + mean_r)
        gap_l, gap_r = mean_l - row_mean, mean_r - row_mean
        deviation = left[base + 8 : base + 16] + right[base + 8 : base + 16]
        spread = (deviation + share * (gap_l * gap_l + gap_r * gap_r)) / bin_total
        scale = jnp.sqrt(spread + EPSILON)
        rows.append((left[:base] + right[:base] - HARM * row_mean[0:1]) / scale[0:1])
    highest = jnp.maximum(rows[0], rows[1])
    level = (rows[0] + rows[1]) / 2
    for column in range(lead):
        block = slice(column * each, (column + 1) * each)
        top[pl.ds(column, each, stride=lead), :] = highest[block]
        level_ref[pl.ds(column, each, stride=lead), :] = level[block]
        for row in range(2):
            harm_ref[pl.ds(2 * column + row, each, stride=2 * lead), :] = rows[row][block]
    for away in range(1, bands):
        peer = lax.rem(band + away, bands)
        third_hop.append(remote(top, peaks.at[band], shards + bands + away, "dm", peer))
        third_hop[-1].start()
    for copy in second_hop + third_hop:
        copy.wait_recv()
    peaks[band] = top[...]
    marks[band] = mark_ref[band]
    peaks_ref[...] = peaks[...]
    marks_ref[...] = marks[...]
    for copy in first_hop + second_hop + third_hop:
        copy.wait_send()


def sift_kernel(level_ref, peaks_ref, marks_ref, out_ref):
    bands, slots, width = out_ref.shape
    blocks = level_ref.shape[0]
    ids = lax.broadcasted_iota(jnp.int32, (slots, blocks), 1)
    lanes = lax.broadcasted_iota(jnp.int32, (slots, width), 1)
    for source in range(bands):
        start = marks_ref[source]
        safe = jnp.maximum(start, 0)
        block, offset = safe // LANES, safe % LANES
        excess = peaks_ref[source] - level_ref[...]

        def pick(which):
            hot = jnp.where(ids == which[:, 0:1], 1.0, 0.0)
            return jnp.dot(hot, excess, precision=lax.Precision.HIGHEST, preferred_element_type=jnp.float32)

        lower, upper = pick(block), pick(block + 1)
        place = lanes + offset
        index = place % LANES
        joined = jnp.where(
            place < LANES, jnp.take_along_axis(lower, index, axis=1), jnp.take_along_axis(upper, index, axis=1)
        )
        out_ref[source] = jnp.where(start >= 0, joined, 0.0)


def fast_device(tables, series, cand_start, cand_count):
    first, twist_tab, second = tables
    dm_rows, samples_dev = series.shape
    shards, bands = lax.axis_size("tm"), lax.axis_size("dm")
    inner, cores = NT // N1, 2
    res, coarse, kept = N1 // cores, N1 // shards, inner // 2
    size = samples_dev // LANES
    cycles = NT // (2 * HARM) // N1
    each, lead = cycles // shards, N1 // LANES
    steps = HARM * (HARM + 1) // 2
    slots = cand_start.shape[3]
    vmem, anywhere = pl.BlockSpec(memory_space=pltpu.VMEM), pl.BlockSpec(memory_space=pl.ANY)
    lined = series.reshape(dm_rows, size, LANES).swapaxes(0, 1).reshape(size * dm_rows, LANES)
    width = lead * each + 16
    moved = pl.pallas_call(
        spectrum_kernel,
        out_shape=jax.ShapeDtypeStruct((shards, width, LANES), jnp.float32),
        in_specs=[vmem, anywhere, anywhere, anywhere],
        out_specs=vmem,
        scratch_shapes=[
            pltpu.VMEM((shards, size, LANES), jnp.float32),
            pltpu.VMEM((size, LANES), jnp.float32),
            pltpu.VMEM((3 * coarse, inner), jnp.bfloat16),
            pltpu.VMEM(first.shape[1:], jnp.bfloat16),
            pltpu.VMEM(twist_tab.shape[1:], jnp.float32),
            pltpu.VMEM(second.shape, jnp.bfloat16),
            pltpu.VMEM((2 * res, inner), jnp.float32),
            pltpu.VMEM((2 * res, inner), jnp.bfloat16),
            pltpu.VMEM((2 * res, inner), jnp.bfloat16),
            pltpu.VMEM((res // LANES, kept, LANES), jnp.float32),
            pltpu.VMEM((2 * cycles, steps * res), jnp.bfloat16),
            pltpu.VMEM((steps * res, N1), jnp.bfloat16),
            pltpu.SemaphoreType.DMA((3,)),
            pltpu.SemaphoreType.DMA((1 + 2 * CHUNKS,)),
            pltpu.SemaphoreType.DMA((1 + 2 * CHUNKS,)),
        ],
        compiler_params=pltpu.CompilerParams(
            collective_id=0, has_side_effects=True, vmem_limit_bytes=VMEM_LIMIT
        ),
    )(lined, jnp.asarray(first), jnp.asarray(twist_tab), jnp.asarray(second))
    live = jnp.arange(slots, dtype=jnp.int32)[None, :] < cand_count[0, 0][:, None]
    marks = jnp.where(live, cand_start[0, 0], -1)
    marks = jnp.broadcast_to(marks[..., None], (bands, slots, LANES))
    blocks = lead * each
    harm, level, peaks, marks_in = pl.pallas_call(
        exchange_kernel,
        out_shape=(
            jax.ShapeDtypeStruct((dm_rows * blocks, LANES), jnp.float32),
            jax.ShapeDtypeStruct((blocks, LANES), jnp.float32),
            jax.ShapeDtypeStruct((bands, blocks, LANES), jnp.float32),
            jax.ShapeDtypeStruct((bands, slots, LANES), jnp.int32),
        ),
        in_specs=[vmem, vmem],
        out_specs=(vmem,) * 4,
        scratch_shapes=[
            pltpu.VMEM((shards, width, LANES), jnp.float32),
            pltpu.VMEM((bands, slots, LANES), jnp.int32),
            pltpu.VMEM((bands, blocks, LANES), jnp.float32),
            pltpu.VMEM((blocks, LANES), jnp.float32),
            pltpu.SemaphoreType.DMA((shards + 2 * bands,)),
            pltpu.SemaphoreType.DMA((shards + 2 * bands,)),
        ],
        compiler_params=pltpu.CompilerParams(collective_id=1, has_side_effects=True),
    )(moved, marks)
    sifted = pl.pallas_call(
        sift_kernel,
        out_shape=jax.ShapeDtypeStruct((bands, slots, BW), jnp.float32),
        in_specs=[vmem] * 3,
        out_specs=vmem,
    )(level, peaks, marks_in)
    harmonic_sum = harm.reshape(blocks, dm_rows, LANES).swapaxes(0, 1).reshape(dm_rows, blocks * LANES)
    return (harmonic_sum, sifted[None, None])


def fits(mesh):
    return mesh.shape["tm"] == 4 and BW == LANES


def solution(mesh):
    if fits(mesh):
        tables = dft_tables(mesh.shape["tm"], 2)

        def body(series, cand_start, cand_count):
            if series.shape[0] != 2:
                return per_device(series, cand_start, cand_count)
            return fast_device(tables, series, cand_start, cand_count)
    else:
        body = per_device
    return jax.shard_map(
        body,
        mesh=mesh,
        in_specs=(
            P(("beam", "dm"), "tm"),
            P(("beam", "tm"), "dm", None, None),
            P(("beam", "tm"), "dm", None),
        ),
        out_specs=(P(("beam", "dm"), "tm"), P(("beam", "tm"), "dm", None, None, None)),
        check_vma=False,
    )
```

```python
import math

import jax
import jax.numpy as jnp
import numpy as np
from jax import lax
from jax.experimental import pallas as pl
from jax.experimental.pallas import tpu as pltpu
from jax.sharding import PartitionSpec as P

NT = 524288
N1 = 512
HARM = 8
BW = 128


EPSILON = 1e-06


def contract(pattern, left, right):
    return jnp.einsum(pattern, left, right, precision=lax.Precision.HIGHEST)


def phase_table(left, right, period):
    turns = left[:, None] * right[None, :] % period
    angle = turns.astype(jnp.float32) * (2.0 * math.pi / period)
    return (jnp.cos(angle), jnp.sin(angle))


def twist(real_part, imag_part, cos_twist, sin_twist):
    return (
        real_part * cos_twist + imag_part * sin_twist,
        imag_part * cos_twist - real_part * sin_twist,
    )


def locate_column(column, per_shard):
    return (column // per_shard, column % per_shard)


def harmonic_tables(column_count, shards, per_shard, harmonics):
    listing = [[[] for harmonic in range(harmonics)] for holder in range(shards)]
    for harmonic in range(1, harmonics + 1):
        for residue in range(column_count):
            product = harmonic * residue
            holder, position = locate_column(product % column_count, per_shard)
            listing[holder][harmonic - 1].append((residue, position, product // column_count))
    slot_width = max((max((len(entries) for entries in group)) for group in listing))
    residue_tab = np.zeros((shards, harmonics, slot_width), np.int32)
    position_tab = np.zeros((shards, harmonics, slot_width), np.int32)
    base_tab = np.zeros((shards, harmonics, slot_width), np.int32)
    valid_tab = np.zeros((shards, harmonics, slot_width), np.float32)
    for holder in range(shards):
        for index in range(harmonics):
            for slot, entry in enumerate(listing[holder][index]):
                residue_tab[holder, index, slot] = entry[0]
                position_tab[holder, index, slot] = entry[1]
                base_tab[holder, index, slot] = entry[2]
                valid_tab[holder, index, slot] = 1.0
    return (residue_tab, position_tab, base_tab, valid_tab)


def per_device(series, cand_start, cand_count):
    dm_rows, samples_dev = series.shape
    shards = lax.axis_size("tm")
    my_index = lax.axis_index("tm")
    inner_len = NT // N1
    kept_bins = inner_len // 2
    per_shard = N1 // shards
    columns = jnp.arange(N1, dtype=jnp.int32)
    coarse_rows = samples_dev // inner_len
    rows_local = series.reshape(dm_rows, coarse_rows, inner_len)
    cos_first, sin_first = phase_table(columns, columns, N1)
    narrow = inner_len // shards
    inner_ids = my_index * narrow + jnp.arange(narrow, dtype=jnp.int32)
    cos_twist, sin_twist = phase_table(inner_ids, columns, NT)
    samples = lax.all_to_all(rows_local, "tm", split_axis=2, concat_axis=1, tiled=True)
    real_part = contract("nab,ar->nbr", samples, cos_first)
    imag_part = -contract("nab,ar->nbr", samples, sin_first)
    twist_re, twist_im = twist(real_part, imag_part, cos_twist, sin_twist)
    cos_second, sin_second = phase_table(
        jnp.arange(inner_len, dtype=jnp.int32), jnp.arange(kept_bins, dtype=jnp.int32), inner_len
    )
    part_re = lax.all_to_all(twist_re, "tm", split_axis=2, concat_axis=1, tiled=True)
    part_im = lax.all_to_all(twist_im, "tm", split_axis=2, concat_axis=1, tiled=True)
    x_re = contract("nbr,bk->nrk", part_re, cos_second) + contract(
        "nbr,bk->nrk", part_im, sin_second
    )
    x_im = contract("nbr,bk->nrk", part_im, cos_second) - contract(
        "nbr,bk->nrk", part_re, sin_second
    )
    power_bins = (x_re * x_re + x_im * x_im) / NT
    bin_total = NT // 2
    row_mean = lax.psum(jnp.sum(power_bins, axis=(1, 2)), "tm") / bin_total
    centered = power_bins - row_mean[:, None, None]
    spread = lax.psum(jnp.sum(centered * centered, axis=(1, 2)), "tm") / bin_total
    scores = centered / jnp.sqrt(spread + EPSILON)[:, None, None]
    score_flat = scores.reshape(dm_rows, per_shard * kept_bins)
    cycles = NT // (2 * HARM) // N1
    residue_tab, position_tab, base_tab, valid_tab = harmonic_tables(N1, shards, per_shard, HARM)
    my_positions = jnp.asarray(position_tab)[my_index]
    my_bases = jnp.asarray(base_tab)[my_index]
    my_valid = jnp.asarray(valid_tab)[my_index]
    cycle_ids = jnp.arange(cycles, dtype=jnp.int32)
    picked_parts = []
    for harmonic in range(1, HARM + 1):
        flat_index = (
            my_positions[harmonic - 1][:, None] * kept_bins
            + my_bases[harmonic - 1][:, None]
            + harmonic * cycle_ids[None, :]
        )
        values = jnp.take(score_flat, flat_index.reshape(-1), axis=1).reshape(dm_rows, -1, cycles)
        picked_parts.append(values * my_valid[harmonic - 1][None, :, None])
    picked = jnp.stack(picked_parts, axis=1)
    my_residues = jnp.asarray(residue_tab)[my_index].reshape(-1)
    spread_values = jnp.swapaxes(picked.reshape(dm_rows, -1, cycles), 1, 2)
    dense = jnp.zeros((dm_rows, cycles, N1), jnp.float32).at[:, :, my_residues].add(spread_values)
    dense = dense.reshape(dm_rows, cycles * N1)
    summed = lax.psum_scatter(dense.T, "tm", scatter_dimension=0, tiled=True)
    harmonic_sum = summed.T
    slot_total = cand_start.shape[3]
    offsets = jnp.arange(BW, dtype=jnp.int32)
    starts = cand_start[0, 0]
    counts = cand_count[0, 0]
    live_slots = jnp.arange(slot_total, dtype=jnp.int32)[None, :] < counts[:, None]
    markers = jnp.where(live_slots, starts, -1).astype(jnp.float32)
    bin_spans = starts[..., None] + offsets
    band_level = jnp.sum(harmonic_sum, axis=0) / dm_rows
    gathered = jnp.take(harmonic_sum, bin_spans, axis=1)
    blocks = jnp.moveaxis(gathered, 0, 2)
    blocks_in = lax.all_to_all(blocks, "dm", split_axis=0, concat_axis=0, tiled=True)
    markers_in = lax.all_to_all(markers, "dm", split_axis=0, concat_axis=0, tiled=True)
    chosen = markers_in.astype(jnp.int32)
    level = jnp.take(band_level, jnp.maximum(chosen, 0)[..., None] + offsets, axis=0)
    sifted = jnp.where(chosen[..., None] >= 0, jnp.max(blocks_in, axis=2) - level, 0.0)
    return (harmonic_sum, sifted[None, None])


MESH = pl.DeviceIdType.MESH
LANES = 128
CHUNKS = 4
VMEM_LIMIT = 60 * 1024 * 1024


def split_pair(value):
    high = value.astype(jnp.bfloat16)
    return high, (value - high.astype(jnp.float32)).astype(jnp.bfloat16)


def host_split(table):
    high = table.astype(jnp.bfloat16)
    low = (table - high.astype(np.float64)).astype(jnp.bfloat16)
    return high, low


def dft_tables(shards):
    inner = NT // N1
    kept = inner // 2
    piece = N1 // shards // CHUNKS
    res = N1 // 2
    ids = np.arange(res)
    first = np.empty((shards // 2, CHUNKS, 2 * res, shards // 2, 2, piece), jnp.bfloat16)
    for shard in range(shards):
        for chunk in range(CHUNKS):
            coarse = (shard * CHUNKS + chunk) * piece + np.arange(piece)
            turn = 2.0 * np.pi * (np.outer(ids, coarse) % N1) / N1
            pair = host_split(np.concatenate([np.cos(turn), -np.sin(turn)], axis=0))
            for part in range(2):
                first[shard // 2, chunk, :, shard % 2, part] = pair[part]
    first = first.reshape(shards // 2, CHUNKS, 2 * res, 2 * shards // 2 * piece)

    def waves(turn):
        return np.stack([np.cos(turn), np.sin(turn)], axis=0).astype(np.float32)

    lanes = np.arange(LANES)
    twists = np.stack(
        [
            waves(2.0 * np.pi * np.outer(ids, lanes) / NT),
            waves(2.0 * np.pi * np.outer(ids, np.full(LANES, LANES)) / NT),
        ],
        axis=0,
    )
    shift = waves(2.0 * np.pi * np.outer(np.full(8, res), lanes) / NT)
    second = np.empty((4, kept, inner // 4), jnp.bfloat16)
    for kind in range(4):
        turn = np.outer(4 * np.arange(kept // 4) + kind, np.arange(inner // 4)) % inner
        turn = 2.0 * np.pi * turn / inner
        cos_pair, sin_pair = host_split(np.cos(turn)), host_split(np.sin(turn))
        second[kind] = np.concatenate([cos_pair[0], sin_pair[0], cos_pair[1], sin_pair[1]], axis=0)
    return first, twists, shift, second


def turned(left, right):
    return left[0] * right[0] - left[1] * right[1], left[0] * right[1] + left[1] * right[0]


def windows(table, start):
    count, blocks = start.shape[0], table.shape[0]
    high = table.astype(jnp.bfloat16)
    rest = table - high.astype(jnp.float32)
    middle = rest.astype(jnp.bfloat16)
    low = (rest - middle.astype(jnp.float32)).astype(jnp.bfloat16)
    block = start // LANES
    ids = lax.broadcasted_iota(jnp.int32, (count, blocks), 1)
    hot = jnp.concatenate(
        [jnp.where(ids == block[:, 0:1], 1.0, 0.0), jnp.where(ids == block[:, 0:1] + 1, 1.0, 0.0)], axis=0
    ).astype(jnp.bfloat16)
    picked = jnp.dot(hot, jnp.concatenate([high, middle, low], axis=1), preferred_element_type=jnp.float32)
    picked = picked[:, 0:LANES] + picked[:, LANES : 2 * LANES] + picked[:, 2 * LANES :]
    place = lax.broadcasted_iota(jnp.int32, (count, LANES), 1) + start % LANES
    index = place % LANES
    return jnp.where(
        place < LANES,
        jnp.take_along_axis(picked[0:count], index, axis=1),
        jnp.take_along_axis(picked[count:], index, axis=1),
    )


def search_kernel(
    x_ref, start_ref, count_ref, first_hbm, twists_ref, shift_ref, second_hbm, harm_ref, sift_ref,
    gathered, outgoing, x_tab, first, twist_tab, second, partial, b_high, b_low, power, picks, select,
    mine, parts, marks_out, marks, tops_out, tops, flat_top, flat_level,
    load_sem, send_sem, recv_sem, hop_send, hop_recv,
):
    me, band = lax.axis_index("tm"), lax.axis_index("dm")
    shards, bands = lax.axis_size("tm"), lax.axis_size("dm")
    core, chip = lax.rem(me, 2), me // 2
    sibling = me + 1 - 2 * core
    across = lax.rem(me + 2, 4)
    size = gathered.shape[1]
    step = size // CHUNKS
    inner = partial.shape[1]
    groups = inner // LANES
    piece_rows = step // groups
    res = partial.shape[0] // 2
    kept = power.shape[1]
    slots = sift_ref.shape[1]

    width = first_hbm.shape[3]
    loads = [
        pltpu.make_async_copy(first_hbm, first.at[:, :, :, pl.ds(0, width)], load_sem.at[0]),
        pltpu.make_async_copy(first_hbm, first.at[:, :, :, pl.ds(width, width)], load_sem.at[1]),
        pltpu.make_async_copy(second_hbm, second, load_sem.at[2]),
    ]
    for load in loads:
        load.start()
    barrier = pltpu.get_barrier_semaphore()
    for axis, count, here in (("tm", shards, me), ("dm", bands, band)):
        for away in range(1, count):
            peer = lax.rem(here + away, count)
            pl.semaphore_signal(barrier, inc=1, device_id={axis: peer}, device_id_type=MESH)
    for piece in range(CHUNKS):
        row_a = x_ref[pl.ds(2 * piece * step, step, stride=2), :]
        row_b = x_ref[pl.ds(2 * piece * step + 1, step, stride=2), :]
        outgoing[piece * step : (piece + 1) * step, :] = jnp.where(chip == 0, row_b, row_a)
        gathered[me, piece * step : (piece + 1) * step, :] = jnp.where(chip == 0, row_a, row_b)
    diagonal_ids = lax.broadcasted_iota(jnp.int32, (slots, slots), 0)
    lane_slots = lax.broadcasted_iota(jnp.int32, (slots, slots), 1)
    for target in range(bands):
        line = jnp.where(
            lane_slots[0:1] < count_ref[0:1, target : target + 1], start_ref[target : target + 1, :], -1
        ).astype(jnp.float32)
        column = jnp.sum(jnp.where(diagonal_ids == lane_slots, line, 0.0), axis=1, keepdims=True)
        marks_out[target] = jnp.broadcast_to(column, (slots, LANES)).astype(jnp.int32)
    pl.semaphore_wait(barrier, shards + bands - 2)

    def remote(src, dst, sems, index, axis, peer):
        return pltpu.make_async_remote_copy(
            src_ref=src, dst_ref=dst, send_sem=sems[0].at[index], recv_sem=sems[1].at[index],
            device_id={axis: peer}, device_id_type=MESH,
        )

    row_sems, hop_sems = (send_sem, recv_sem), (hop_send, hop_recv)
    crossing = []
    for piece in range(CHUNKS):
        rows = pl.ds(piece * step, step)
        crossing.append(remote(outgoing.at[rows], gathered.at[me, rows], row_sems, 1 + piece, "tm", across))
        crossing[-1].start()
    own = remote(gathered.at[me], gathered.at[me], row_sems, 0, "tm", sibling)
    own.start()
    mark_hop, part_hop, top_hop = [], [], []
    for away in range(1, bands):
        peer = lax.rem(band + away, bands)
        mark_hop.append(remote(marks_out.at[peer], marks.at[band], hop_sems, shards + away, "dm", peer))
        mark_hop[-1].start()

    odd_core = core == 1
    shifted = (jnp.where(odd_core, shift_ref[0, 0:1], 1.0), jnp.where(odd_core, shift_ref[1, 0:1], 0.0))
    corner = 2.0 * math.pi * LANES * res / NT
    bent = (jnp.where(odd_core, math.cos(corner), 1.0), jnp.where(odd_core, math.sin(corner), 0.0))
    running = turned((twists_ref[0, 0], twists_ref[0, 1]), shifted)
    advance = turned((twists_ref[1, 0], twists_ref[1, 1]), bent)
    for group in range(groups):
        cols = slice(group * LANES, (group + 1) * LANES)
        twist_tab[0, :, cols], twist_tab[1, :, cols] = running
        if group + 1 < groups:
            running = turned(running, advance)

    for load in loads:
        load.wait()
    parity = lax.broadcasted_iota(jnp.int32, (piece_rows, LANES), 0) % 2
    sign = jnp.where(jnp.logical_and(parity == 1, odd_core), -1.0, 1.0)

    def accumulate(side, piece, fresh):
        for group in range(groups):
            cols = slice(group * LANES, (group + 1) * LANES)
            for half in range(2):
                taken = gathered[2 * side + half, pl.ds(piece * step + group, piece_rows, stride=groups), :]
                pair = split_pair(taken * sign)
                for part in range(2):
                    base = (4 * part + 2 * half) * piece_rows
                    x_tab[base : base + piece_rows, cols] = pair[part]
                    x_tab[base + piece_rows : base + 2 * piece_rows, cols] = pair[part]
        for block in range(inner // 256):
            cols = slice(block * 256, (block + 1) * 256)
            term = jnp.dot(first[side, piece], x_tab[:, cols], preferred_element_type=jnp.float32)
            partial[:, cols] = term if fresh else partial[:, cols] + term

    own.wait_recv()
    for piece in range(CHUNKS):
        accumulate(chip, piece, piece == 0)

    lane_ids = lax.broadcasted_iota(jnp.int32, (res, res), 1)
    res_ids = lax.broadcasted_iota(jnp.int32, (res, res), 0) + core * res
    plan = []
    slot = 0
    for harmonic in range(1, HARM + 1):
        depth = (harmonic + 1) // 2
        plan.append((harmonic, depth, slot))
        for tile in range(2):
            target = (lane_ids + tile * res) * harmonic - res_ids
            for index in range(depth):
                cycle = index if tile == 0 else harmonic - depth + index
                hit = jnp.where(target == cycle * N1, 1.0, 0.0)
                select[tile, (slot + index) * res : (slot + index + 1) * res, :] = hit.astype(jnp.bfloat16)
        slot += depth

    forwards = []
    for piece in range(CHUNKS):
        rows = pl.ds(piece * step, step)
        crossing[piece].wait_recv()
        forwards.append(
            remote(gathered.at[across, rows], gathered.at[across, rows], row_sems, 1 + CHUNKS + piece, "tm", sibling)
        )
        forwards[-1].start()
        if piece > 0:
            forwards[piece - 1].wait_recv()
            accumulate(1 - chip, piece - 1, False)
    forwards[-1].wait_recv()
    accumulate(1 - chip, CHUNKS - 1, False)

    quarter = inner // 4

    def twisted(block):
        cols = slice(block * LANES, (block + 1) * LANES)
        return twist(
            partial[0:res, cols], partial[res : 2 * res, cols], twist_tab[0, :, cols], twist_tab[1, :, cols]
        )

    for block in range(quarter // LANES):
        quads = [twisted(block + turn * (quarter // LANES)) for turn in range(4)]
        even_re, even_im = quads[0][0] + quads[2][0], quads[0][1] + quads[2][1]
        odd_re, odd_im = quads[1][0] + quads[3][0], quads[1][1] + quads[3][1]
        gap_re, gap_im = quads[0][0] - quads[2][0], quads[0][1] - quads[2][1]
        lag_re, lag_im = quads[1][0] - quads[3][0], quads[1][1] - quads[3][1]
        cols = slice(block * LANES, (block + 1) * LANES)
        for kind, value in enumerate(
            (
                (even_re + odd_re, even_im + odd_im),
                (gap_re + lag_im, gap_im - lag_re),
                (even_re - odd_re, even_im - odd_im),
                (gap_re - lag_im, gap_im + lag_re),
            )
        ):
            for part in range(2):
                rows = slice(part * res, (part + 1) * res)
                b_high[kind, rows, cols], b_low[kind, rows, cols] = split_pair(value[part])

    def against(table, right):
        return lax.dot_general(table, right, (((1,), (1,)), ((), ())), preferred_element_type=jnp.float32)

    fourth = kept // 4
    total = jnp.zeros((1, 1), jnp.float32)
    for kind in range(4):
        both = against(second[kind], b_high[kind])
        less = against(second[kind, 0 : 2 * fourth], b_low[kind])
        by_cos = both[0:fourth] + both[2 * fourth : 3 * fourth] + less[0:fourth]
        by_sin = both[fourth : 2 * fourth] + both[3 * fourth :] + less[fourth:]
        x_re = by_cos[:, 0:res] + by_sin[:, res:]
        x_im = by_cos[:, res:] - by_sin[:, 0:res]
        bins = (x_re * x_re + x_im * x_im) / NT
        total = total + jnp.sum(jnp.sum(bins, axis=0, keepdims=True), axis=1, keepdims=True)
        for column in range(res // LANES):
            power[column, pl.ds(kind, fourth, stride=4), :] = bins[:, column * LANES : (column + 1) * LANES]

    cycles = NT // (2 * HARM) // N1
    sums = [jnp.zeros((2 * cycles, res), jnp.float32) for tile in range(2)]
    slot = 0
    for harmonic, depth, base in plan:
        for cycle in range(harmonic):
            for column in range(res // LANES):
                high, low = split_pair(power[column, pl.ds(cycle, cycles, stride=harmonic), :])
                cols = slice((slot + cycle) * res + column * LANES, (slot + cycle) * res + (column + 1) * LANES)
                picks[0:cycles, cols] = high
                picks[cycles : 2 * cycles, cols] = low
        for tile in range(2):
            begin = (slot + (0 if tile == 0 else harmonic - depth)) * res
            sums[tile] = sums[tile] + jnp.dot(
                picks[:, begin : begin + depth * res],
                select[tile, base * res : (base + depth) * res, :],
                preferred_element_type=jnp.float32,
            )
        slot += harmonic
    mean = total / (kept * res)
    off = power[...] - mean[None]
    deviation = jnp.sum(jnp.sum(jnp.sum(off * off, axis=0), axis=0, keepdims=True), axis=1, keepdims=True)
    mean = jnp.broadcast_to(mean, (8, LANES))
    deviation = jnp.broadcast_to(deviation, (8, LANES))
    each, lead = cycles // shards, N1 // LANES
    base = lead * each
    for shard in range(shards):
        for column in range(lead):
            found = sums[column * LANES // res][:, column * LANES % res : column * LANES % res + LANES]
            mine[shard, column * each : (column + 1) * each, :] = (
                found[shard * each : (shard + 1) * each] + found[cycles + shard * each : cycles + (shard + 1) * each]
            )
        mine[shard, base : base + 8, :] = mean
        mine[shard, base + 8 : base + 16, :] = deviation
    for away in range(1, shards):
        peer = lax.rem(me + away, shards)
        part_hop.append(remote(mine.at[peer], parts.at[me], hop_sems, away, "tm", peer))
        part_hop[-1].start()
    parts[me] = mine[me]
    marks[band] = marks_out[band]
    for copy in part_hop:
        copy.wait_recv()

    bin_total = NT // 2
    share = bin_total // 2
    found = []
    for row in range(2):
        left, right = parts[2 * row], parts[2 * row + 1]
        mean_l, mean_r = left[base : base + 8], right[base : base + 8]
        row_mean = 0.5 * (mean_l + mean_r)
        gap_l, gap_r = mean_l - row_mean, mean_r - row_mean
        squares = left[base + 8 : base + 16] + right[base + 8 : base + 16]
        spread = (squares + share * (gap_l * gap_l + gap_r * gap_r)) / bin_total
        scale = jnp.sqrt(spread + EPSILON)
        found.append((left[:base] + right[:base] - HARM * row_mean[0:1]) / scale[0:1])
    highest = jnp.maximum(found[0], found[1])
    level = (found[0] + found[1]) / 2
    for column in range(lead):
        block = slice(column * each, (column + 1) * each)
        flat_top[pl.ds(column, each, stride=lead), :] = highest[block]
        flat_level[pl.ds(column, each, stride=lead), :] = level[block]
        for row in range(2):
            harm_ref[pl.ds(2 * column + row, each, stride=2 * lead), :] = found[row][block]
    sent = jnp.maximum(marks_out[...].reshape(bands * slots, LANES), 0)
    tops_out[...] = windows(flat_top[...], sent).reshape(bands, slots, LANES)
    for away in range(1, bands):
        peer = lax.rem(band + away, bands)
        top_hop.append(remote(tops_out.at[peer], tops.at[band], hop_sems, shards + bands + away, "dm", peer))
        top_hop[-1].start()
    tops[band] = tops_out[band]
    for copy in mark_hop:
        copy.wait_recv()
    wanted = marks[...].reshape(bands * slots, LANES)
    floor = windows(flat_level[...], jnp.maximum(wanted, 0)).reshape(bands, slots, LANES)
    for copy in top_hop:
        copy.wait_recv()
    sift_ref[...] = jnp.where(marks[...] >= 0, tops[...] - floor, 0.0)
    own.wait_send()
    for copy in crossing + forwards + mark_hop + part_hop + top_hop:
        copy.wait_send()


def fast_device(tables, series, cand_start, cand_count):
    first, twists, shift, second = tables
    dm_rows, samples_dev = series.shape
    shards, bands = lax.axis_size("tm"), lax.axis_size("dm")
    inner, res = NT // N1, N1 // 2
    kept = inner // 2
    size = samples_dev // LANES
    cycles = NT // (2 * HARM) // N1
    each, lead = cycles // shards, N1 // LANES
    steps = HARM * (HARM + 1) // 2
    depth = sum((harmonic + 1) // 2 for harmonic in range(1, HARM + 1))
    slots = cand_start.shape[3]
    blocks = lead * each
    width = blocks + 16
    vmem, anywhere = pl.BlockSpec(memory_space=pltpu.VMEM), pl.BlockSpec(memory_space=pl.ANY)
    lined = series.reshape(dm_rows, size, LANES).swapaxes(0, 1).reshape(size * dm_rows, LANES)
    low, wide = jnp.bfloat16, jnp.float32
    harm, sifted = pl.pallas_call(
        search_kernel,
        out_shape=(
            jax.ShapeDtypeStruct((dm_rows * blocks, LANES), wide),
            jax.ShapeDtypeStruct((bands, slots, LANES), wide),
        ),
        in_specs=[vmem, vmem, vmem, anywhere, vmem, vmem, anywhere],
        out_specs=(vmem, vmem),
        scratch_shapes=[
            pltpu.VMEM((shards, size, LANES), wide),
            pltpu.VMEM((size, LANES), wide),
            pltpu.VMEM((2 * first.shape[3], inner), low),
            pltpu.VMEM(first.shape[:3] + (2 * first.shape[3],), low),
            pltpu.VMEM((2, res, inner), wide),
            pltpu.VMEM(second.shape, low),
            pltpu.VMEM((2 * res, inner), wide),
            pltpu.VMEM((4, 2 * res, inner // 4), low),
            pltpu.VMEM((4, 2 * res, inner // 4), low),
            pltpu.VMEM((res // LANES, kept, LANES), wide),
            pltpu.VMEM((2 * cycles, steps * res), low),
            pltpu.VMEM((2, depth * res, res), low),
            pltpu.VMEM((shards, width, LANES), wide),
            pltpu.VMEM((shards, width, LANES), wide),
            pltpu.VMEM((bands, slots, LANES), jnp.int32),
            pltpu.VMEM((bands, slots, LANES), jnp.int32),
            pltpu.VMEM((bands, slots, LANES), wide),
            pltpu.VMEM((bands, slots, LANES), wide),
            pltpu.VMEM((blocks, LANES), wide),
            pltpu.VMEM((blocks, LANES), wide),
            pltpu.SemaphoreType.DMA((3,)),
            pltpu.SemaphoreType.DMA((1 + 2 * CHUNKS,)),
            pltpu.SemaphoreType.DMA((1 + 2 * CHUNKS,)),
            pltpu.SemaphoreType.DMA((shards + 2 * bands,)),
            pltpu.SemaphoreType.DMA((shards + 2 * bands,)),
        ],
        compiler_params=pltpu.CompilerParams(
            collective_id=0, has_side_effects=True, vmem_limit_bytes=VMEM_LIMIT
        ),
    )(
        lined, cand_start[0, 0], cand_count[0], jnp.asarray(first), jnp.asarray(twists), jnp.asarray(shift),
        jnp.asarray(second),
    )
    harmonic_sum = harm.reshape(blocks, dm_rows, LANES).swapaxes(0, 1).reshape(dm_rows, blocks * LANES)
    return (harmonic_sum, sifted[None, None])


def fits(mesh):
    return mesh.shape["tm"] == 4 and BW == LANES


def solution(mesh):
    if fits(mesh):
        tables = dft_tables(mesh.shape["tm"])

        def body(series, cand_start, cand_count):
            if series.shape[0] != 2:
                return per_device(series, cand_start, cand_count)
            return fast_device(tables, series, cand_start, cand_count)
    else:
        body = per_device
    return jax.shard_map(
        body,
        mesh=mesh,
        in_specs=(
            P(("beam", "dm"), "tm"),
            P(("beam", "tm"), "dm", None, None),
            P(("beam", "tm"), "dm", None),
        ),
        out_specs=(P(("beam", "dm"), "tm"), P(("beam", "tm"), "dm", None, None, None)),
        check_vma=False,
    )
```

```python
import math

import jax
import jax.numpy as jnp
import numpy as np
from jax import lax
from jax.experimental import pallas as pl
from jax.experimental.pallas import tpu as pltpu
from jax.sharding import PartitionSpec as P

NT = 524288
N1 = 512
HARM = 8
BW = 128


EPSILON = 1e-06


def contract(pattern, left, right):
    return jnp.einsum(pattern, left, right, precision=lax.Precision.HIGHEST)


def phase_table(left, right, period):
    turns = left[:, None] * right[None, :] % period
    angle = turns.astype(jnp.float32) * (2.0 * math.pi / period)
    return (jnp.cos(angle), jnp.sin(angle))


def twist(real_part, imag_part, cos_twist, sin_twist):
    return (
        real_part * cos_twist + imag_part * sin_twist,
        imag_part * cos_twist - real_part * sin_twist,
    )


def locate_column(column, per_shard):
    return (column // per_shard, column % per_shard)


def harmonic_tables(column_count, shards, per_shard, harmonics):
    listing = [[[] for harmonic in range(harmonics)] for holder in range(shards)]
    for harmonic in range(1, harmonics + 1):
        for residue in range(column_count):
            product = harmonic * residue
            holder, position = locate_column(product % column_count, per_shard)
            listing[holder][harmonic - 1].append((residue, position, product // column_count))
    slot_width = max((max((len(entries) for entries in group)) for group in listing))
    residue_tab = np.zeros((shards, harmonics, slot_width), np.int32)
    position_tab = np.zeros((shards, harmonics, slot_width), np.int32)
    base_tab = np.zeros((shards, harmonics, slot_width), np.int32)
    valid_tab = np.zeros((shards, harmonics, slot_width), np.float32)
    for holder in range(shards):
        for index in range(harmonics):
            for slot, entry in enumerate(listing[holder][index]):
                residue_tab[holder, index, slot] = entry[0]
                position_tab[holder, index, slot] = entry[1]
                base_tab[holder, index, slot] = entry[2]
                valid_tab[holder, index, slot] = 1.0
    return (residue_tab, position_tab, base_tab, valid_tab)


def per_device(series, cand_start, cand_count):
    dm_rows, samples_dev = series.shape
    shards = lax.axis_size("tm")
    my_index = lax.axis_index("tm")
    inner_len = NT // N1
    kept_bins = inner_len // 2
    per_shard = N1 // shards
    columns = jnp.arange(N1, dtype=jnp.int32)
    coarse_rows = samples_dev // inner_len
    rows_local = series.reshape(dm_rows, coarse_rows, inner_len)
    cos_first, sin_first = phase_table(columns, columns, N1)
    narrow = inner_len // shards
    inner_ids = my_index * narrow + jnp.arange(narrow, dtype=jnp.int32)
    cos_twist, sin_twist = phase_table(inner_ids, columns, NT)
    samples = lax.all_to_all(rows_local, "tm", split_axis=2, concat_axis=1, tiled=True)
    real_part = contract("nab,ar->nbr", samples, cos_first)
    imag_part = -contract("nab,ar->nbr", samples, sin_first)
    twist_re, twist_im = twist(real_part, imag_part, cos_twist, sin_twist)
    cos_second, sin_second = phase_table(
        jnp.arange(inner_len, dtype=jnp.int32), jnp.arange(kept_bins, dtype=jnp.int32), inner_len
    )
    part_re = lax.all_to_all(twist_re, "tm", split_axis=2, concat_axis=1, tiled=True)
    part_im = lax.all_to_all(twist_im, "tm", split_axis=2, concat_axis=1, tiled=True)
    x_re = contract("nbr,bk->nrk", part_re, cos_second) + contract(
        "nbr,bk->nrk", part_im, sin_second
    )
    x_im = contract("nbr,bk->nrk", part_im, cos_second) - contract(
        "nbr,bk->nrk", part_re, sin_second
    )
    power_bins = (x_re * x_re + x_im * x_im) / NT
    bin_total = NT // 2
    row_mean = lax.psum(jnp.sum(power_bins, axis=(1, 2)), "tm") / bin_total
    centered = power_bins - row_mean[:, None, None]
    spread = lax.psum(jnp.sum(centered * centered, axis=(1, 2)), "tm") / bin_total
    scores = centered / jnp.sqrt(spread + EPSILON)[:, None, None]
    score_flat = scores.reshape(dm_rows, per_shard * kept_bins)
    cycles = NT // (2 * HARM) // N1
    residue_tab, position_tab, base_tab, valid_tab = harmonic_tables(N1, shards, per_shard, HARM)
    my_positions = jnp.asarray(position_tab)[my_index]
    my_bases = jnp.asarray(base_tab)[my_index]
    my_valid = jnp.asarray(valid_tab)[my_index]
    cycle_ids = jnp.arange(cycles, dtype=jnp.int32)
    picked_parts = []
    for harmonic in range(1, HARM + 1):
        flat_index = (
            my_positions[harmonic - 1][:, None] * kept_bins
            + my_bases[harmonic - 1][:, None]
            + harmonic * cycle_ids[None, :]
        )
        values = jnp.take(score_flat, flat_index.reshape(-1), axis=1).reshape(dm_rows, -1, cycles)
        picked_parts.append(values * my_valid[harmonic - 1][None, :, None])
    picked = jnp.stack(picked_parts, axis=1)
    my_residues = jnp.asarray(residue_tab)[my_index].reshape(-1)
    spread_values = jnp.swapaxes(picked.reshape(dm_rows, -1, cycles), 1, 2)
    dense = jnp.zeros((dm_rows, cycles, N1), jnp.float32).at[:, :, my_residues].add(spread_values)
    dense = dense.reshape(dm_rows, cycles * N1)
    summed = lax.psum_scatter(dense.T, "tm", scatter_dimension=0, tiled=True)
    harmonic_sum = summed.T
    slot_total = cand_start.shape[3]
    offsets = jnp.arange(BW, dtype=jnp.int32)
    starts = cand_start[0, 0]
    counts = cand_count[0, 0]
    live_slots = jnp.arange(slot_total, dtype=jnp.int32)[None, :] < counts[:, None]
    markers = jnp.where(live_slots, starts, -1).astype(jnp.float32)
    bin_spans = starts[..., None] + offsets
    band_level = jnp.sum(harmonic_sum, axis=0) / dm_rows
    gathered = jnp.take(harmonic_sum, bin_spans, axis=1)
    blocks = jnp.moveaxis(gathered, 0, 2)
    blocks_in = lax.all_to_all(blocks, "dm", split_axis=0, concat_axis=0, tiled=True)
    markers_in = lax.all_to_all(markers, "dm", split_axis=0, concat_axis=0, tiled=True)
    chosen = markers_in.astype(jnp.int32)
    level = jnp.take(band_level, jnp.maximum(chosen, 0)[..., None] + offsets, axis=0)
    sifted = jnp.where(chosen[..., None] >= 0, jnp.max(blocks_in, axis=2) - level, 0.0)
    return (harmonic_sum, sifted[None, None])


MESH = pl.DeviceIdType.MESH
LANES = 128
CHUNKS = 4
VMEM_LIMIT = 60 * 1024 * 1024


def split_pair(value):
    high = value.astype(jnp.bfloat16)
    return high, (value - high.astype(jnp.float32)).astype(jnp.bfloat16)


def host_split(table):
    high = table.astype(jnp.bfloat16)
    low = (table - high.astype(np.float64)).astype(jnp.bfloat16)
    return high, low


def dft_tables(shards):
    inner = NT // N1
    kept = inner // 2
    piece = N1 // shards // CHUNKS
    res = N1 // 2
    ids = np.arange(res)
    first = np.empty((shards // 2, CHUNKS, 2 * res, shards // 2, 2, piece), jnp.bfloat16)
    for shard in range(shards):
        for chunk in range(CHUNKS):
            coarse = (shard * CHUNKS + chunk) * piece + np.arange(piece)
            turn = 2.0 * np.pi * (np.outer(ids, coarse) % N1) / N1
            pair = host_split(np.concatenate([np.cos(turn), -np.sin(turn)], axis=0))
            for part in range(2):
                first[shard // 2, chunk, :, shard % 2, part] = pair[part]
    first = first.reshape(shards // 2, CHUNKS, 2 * res, 2 * shards // 2 * piece)

    def waves(turn):
        return np.stack([np.cos(turn), np.sin(turn)], axis=0).astype(np.float32)

    lanes = np.arange(LANES)
    twists = np.stack(
        [
            waves(2.0 * np.pi * np.outer(ids, lanes) / NT),
            waves(2.0 * np.pi * np.outer(ids, np.full(LANES, LANES)) / NT),
        ],
        axis=0,
    )
    shift = waves(2.0 * np.pi * np.outer(np.full(8, res), lanes) / NT)
    second = np.empty((4, kept, inner // 4), jnp.bfloat16)
    for kind in range(4):
        turn = np.outer(4 * np.arange(kept // 4) + kind, np.arange(inner // 4)) % inner
        turn = 2.0 * np.pi * turn / inner
        cos_pair, sin_pair = host_split(np.cos(turn)), host_split(np.sin(turn))
        second[kind] = np.concatenate([cos_pair[0], sin_pair[0], cos_pair[1], sin_pair[1]], axis=0)
    return first, twists, shift, second


def turned(left, right):
    return left[0] * right[0] - left[1] * right[1], left[0] * right[1] + left[1] * right[0]


def windows(table, start):
    count, blocks = start.shape[0], table.shape[0]
    high = table.astype(jnp.bfloat16)
    rest = table - high.astype(jnp.float32)
    middle = rest.astype(jnp.bfloat16)
    low = (rest - middle.astype(jnp.float32)).astype(jnp.bfloat16)
    block = start // LANES
    ids = lax.broadcasted_iota(jnp.int32, (count, blocks), 1)
    hot = jnp.concatenate(
        [jnp.where(ids == block[:, 0:1], 1.0, 0.0), jnp.where(ids == block[:, 0:1] + 1, 1.0, 0.0)], axis=0
    ).astype(jnp.bfloat16)
    picked = jnp.dot(hot, jnp.concatenate([high, middle, low], axis=1), preferred_element_type=jnp.float32)
    picked = picked[:, 0:LANES] + picked[:, LANES : 2 * LANES] + picked[:, 2 * LANES :]
    place = lax.broadcasted_iota(jnp.int32, (count, LANES), 1) + start % LANES
    index = place % LANES
    return jnp.where(
        place < LANES,
        jnp.take_along_axis(picked[0:count], index, axis=1),
        jnp.take_along_axis(picked[count:], index, axis=1),
    )


def search_kernel(
    x_hbm, start_ref, count_ref, first_hbm, twists_ref, shift_ref, second_hbm, harm_ref, scale_ref, sift_ref,
    x_ref, gathered, outgoing, x_tab, first, twist_tab, second, partial, b_high, b_low, power, picks, select,
    mine, parts, marks_out, marks, tops_out, tops, flat_top, flat_level,
    load_sem, send_sem, recv_sem, hop_send, hop_recv,
):
    me, band = lax.axis_index("tm"), lax.axis_index("dm")
    shards, bands = lax.axis_size("tm"), lax.axis_size("dm")
    core, chip = lax.rem(me, 2), me // 2
    sibling = me + 1 - 2 * core
    across = lax.rem(me + 2, 4)
    size = gathered.shape[1]
    step = size // CHUNKS
    inner = partial.shape[1]
    groups = inner // LANES
    piece_rows = step // groups
    res = partial.shape[0] // 2
    kept = power.shape[1]
    slots = sift_ref.shape[1]

    barrier = pltpu.get_barrier_semaphore()
    for axis, count, here in (("tm", shards, me), ("dm", bands, band)):
        for away in range(1, count):
            peer = lax.rem(here + away, count)
            pl.semaphore_signal(barrier, inc=1, device_id={axis: peer}, device_id_type=MESH)
    arrivals = []
    for piece in range(CHUNKS):
        rows = pl.ds(2 * piece * step, 2 * step)
        arrivals.append(pltpu.make_async_copy(x_hbm.at[rows], x_ref.at[rows], load_sem.at[3 + piece]))
        arrivals[-1].start()
    width = first_hbm.shape[3]
    loads = [
        pltpu.make_async_copy(first_hbm, first.at[:, :, :, pl.ds(0, width)], load_sem.at[0]),
        pltpu.make_async_copy(first_hbm, first.at[:, :, :, pl.ds(width, width)], load_sem.at[1]),
        pltpu.make_async_copy(second_hbm, second, load_sem.at[2]),
    ]
    for load in loads:
        load.start()
    for piece in range(CHUNKS):
        arrivals[piece].wait()
        row_a = x_ref[pl.ds(2 * piece * step, step, stride=2), :]
        row_b = x_ref[pl.ds(2 * piece * step + 1, step, stride=2), :]
        outgoing[piece * step : (piece + 1) * step, :] = jnp.where(chip == 0, row_b, row_a)
        gathered[me, piece * step : (piece + 1) * step, :] = jnp.where(chip == 0, row_a, row_b)
    diagonal_ids = lax.broadcasted_iota(jnp.int32, (slots, slots), 0)
    lane_slots = lax.broadcasted_iota(jnp.int32, (slots, slots), 1)
    for target in range(bands):
        line = jnp.where(
            lane_slots[0:1] < count_ref[0:1, target : target + 1], start_ref[target : target + 1, :], -1
        ).astype(jnp.float32)
        column = jnp.sum(jnp.where(diagonal_ids == lane_slots, line, 0.0), axis=1, keepdims=True)
        marks_out[target] = jnp.broadcast_to(column, (slots, LANES)).astype(jnp.int32)
    pl.semaphore_wait(barrier, shards + bands - 2)

    def remote(src, dst, sems, index, axis, peer):
        return pltpu.make_async_remote_copy(
            src_ref=src, dst_ref=dst, send_sem=sems[0].at[index], recv_sem=sems[1].at[index],
            device_id={axis: peer}, device_id_type=MESH,
        )

    row_sems, hop_sems = (send_sem, recv_sem), (hop_send, hop_recv)
    crossing = []
    for piece in range(CHUNKS):
        rows = pl.ds(piece * step, step)
        crossing.append(remote(outgoing.at[rows], gathered.at[me, rows], row_sems, 1 + piece, "tm", across))
        crossing[-1].start()
    own = remote(gathered.at[me], gathered.at[me], row_sems, 0, "tm", sibling)
    own.start()
    mark_hop, part_hop, top_hop = [], [], []
    for away in range(1, bands):
        peer = lax.rem(band + away, bands)
        mark_hop.append(remote(marks_out.at[peer], marks.at[band], hop_sems, shards + away, "dm", peer))
        mark_hop[-1].start()

    odd_core = core == 1
    shifted = (jnp.where(odd_core, shift_ref[0, 0:1], 1.0), jnp.where(odd_core, shift_ref[1, 0:1], 0.0))
    corner = 2.0 * math.pi * LANES * res / NT
    bent = (jnp.where(odd_core, math.cos(corner), 1.0), jnp.where(odd_core, math.sin(corner), 0.0))
    running = turned((twists_ref[0, 0], twists_ref[0, 1]), shifted)
    advance = turned((twists_ref[1, 0], twists_ref[1, 1]), bent)
    for group in range(groups):
        cols = slice(group * LANES, (group + 1) * LANES)
        twist_tab[0, :, cols], twist_tab[1, :, cols] = running
        if group + 1 < groups:
            running = turned(running, advance)

    for load in loads:
        load.wait()
    parity = lax.broadcasted_iota(jnp.int32, (piece_rows, LANES), 0) % 2
    sign = jnp.where(jnp.logical_and(parity == 1, odd_core), -1.0, 1.0)

    quads = groups // 4

    def place(group):
        spot = group % quads * 4 + group // quads
        return slice(spot * LANES, (spot + 1) * LANES)

    def prepare(side, piece):
        for group in range(groups):
            cols = place(group)
            for half in range(2):
                taken = gathered[2 * side + half, pl.ds(piece * step + group, piece_rows, stride=groups), :]
                pair = split_pair(taken * sign)
                for part in range(2):
                    base = (4 * part + 2 * half) * piece_rows
                    x_tab[base : base + piece_rows, cols] = pair[part]
                    x_tab[base + piece_rows : base + 2 * piece_rows, cols] = pair[part]

    def multiply(side, piece, fresh, spans):
        for block in spans:
            cols = slice(block * 256, (block + 1) * 256)
            term = jnp.dot(first[side, piece], x_tab[:, cols], preferred_element_type=jnp.float32)
            partial[:, cols] = term if fresh else partial[:, cols] + term

    def accumulate(side, piece, fresh):
        prepare(side, piece)
        multiply(side, piece, fresh, range(inner // 256))

    own.wait_recv()
    for piece in range(CHUNKS):
        accumulate(chip, piece, piece == 0)

    lane_ids = lax.broadcasted_iota(jnp.int32, (res, res), 1)
    res_ids = lax.broadcasted_iota(jnp.int32, (res, res), 0) + core * res
    plan = []
    slot = 0
    for harmonic in range(1, HARM + 1):
        depth = (harmonic + 1) // 2
        plan.append((harmonic, depth, slot))
        for tile in range(2):
            target = (lane_ids + tile * res) * harmonic - res_ids
            for index in range(depth):
                cycle = index if tile == 0 else harmonic - depth + index
                hit = jnp.where(target == cycle * N1, 1.0, 0.0)
                select[tile, (slot + index) * res : (slot + index + 1) * res, :] = hit.astype(jnp.bfloat16)
        slot += depth

    forwards = []
    for piece in range(CHUNKS):
        rows = pl.ds(piece * step, step)
        crossing[piece].wait_recv()
        forwards.append(
            remote(gathered.at[across, rows], gathered.at[across, rows], row_sems, 1 + CHUNKS + piece, "tm", sibling)
        )
        forwards[-1].start()
        if piece > 0:
            forwards[piece - 1].wait_recv()
            accumulate(1 - chip, piece - 1, False)
    forwards[-1].wait_recv()
    prepare(1 - chip, CHUNKS - 1)

    quarter = inner // 4

    def twisted(block):
        cols, spot = slice(block * LANES, (block + 1) * LANES), place(block)
        return twist(
            partial[0:res, spot], partial[res : 2 * res, spot], twist_tab[0, :, cols], twist_tab[1, :, cols]
        )

    for block in range(quarter // LANES):
        multiply(1 - chip, CHUNKS - 1, False, range(2 * block, 2 * block + 2))
        four = [twisted(block + turn * (quarter // LANES)) for turn in range(4)]
        even_re, even_im = four[0][0] + four[2][0], four[0][1] + four[2][1]
        odd_re, odd_im = four[1][0] + four[3][0], four[1][1] + four[3][1]
        gap_re, gap_im = four[0][0] - four[2][0], four[0][1] - four[2][1]
        lag_re, lag_im = four[1][0] - four[3][0], four[1][1] - four[3][1]
        cols = slice(block * LANES, (block + 1) * LANES)
        for kind, value in enumerate(
            (
                (even_re + odd_re, even_im + odd_im),
                (gap_re + lag_im, gap_im - lag_re),
                (even_re - odd_re, even_im - odd_im),
                (gap_re - lag_im, gap_im + lag_re),
            )
        ):
            for part in range(2):
                rows = slice(part * res, (part + 1) * res)
                b_high[kind, rows, cols], b_low[kind, rows, cols] = split_pair(value[part])

    def against(table, right):
        return lax.dot_general(table, right, (((1,), (1,)), ((), ())), preferred_element_type=jnp.float32)

    fourth = kept // 4
    total = jnp.zeros((1, 1), jnp.float32)
    for kind in range(4):
        both = against(second[kind], b_high[kind])
        less = against(second[kind, 0 : 2 * fourth], b_low[kind])
        by_cos = both[0:fourth] + both[2 * fourth : 3 * fourth] + less[0:fourth]
        by_sin = both[fourth : 2 * fourth] + both[3 * fourth :] + less[fourth:]
        x_re = by_cos[:, 0:res] + by_sin[:, res:]
        x_im = by_cos[:, res:] - by_sin[:, 0:res]
        bins = (x_re * x_re + x_im * x_im) / NT
        total = total + jnp.sum(jnp.sum(bins, axis=0, keepdims=True), axis=1, keepdims=True)
        for column in range(res // LANES):
            power[column, pl.ds(kind, fourth, stride=4), :] = bins[:, column * LANES : (column + 1) * LANES]

    cycles = NT // (2 * HARM) // N1
    sums = [jnp.zeros((2 * cycles, res), jnp.float32) for tile in range(2)]
    slot = 0
    for harmonic, depth, base in plan:
        for cycle in range(harmonic):
            for column in range(res // LANES):
                high, low = split_pair(power[column, pl.ds(cycle, cycles, stride=harmonic), :])
                cols = slice((slot + cycle) * res + column * LANES, (slot + cycle) * res + (column + 1) * LANES)
                picks[0:cycles, cols] = high
                picks[cycles : 2 * cycles, cols] = low
        for tile in range(2):
            begin = (slot + (0 if tile == 0 else harmonic - depth)) * res
            sums[tile] = sums[tile] + jnp.dot(
                picks[:, begin : begin + depth * res],
                select[tile, base * res : (base + depth) * res, :],
                preferred_element_type=jnp.float32,
            )
        slot += harmonic
    mean = total / (kept * res)
    off = power[...] - mean[None]
    deviation = jnp.sum(jnp.sum(jnp.sum(off * off, axis=0), axis=0, keepdims=True), axis=1, keepdims=True)
    stat_rows = lax.broadcasted_iota(jnp.int32, (8, LANES), 0)
    stats = jnp.where(stat_rows == 0, mean, deviation)
    each, lead = cycles // shards, N1 // LANES
    base = lead * each
    for shard in range(shards):
        for column in range(lead):
            found = sums[column * LANES // res][:, column * LANES % res : column * LANES % res + LANES]
            mine[shard, column * each : (column + 1) * each, :] = (
                found[shard * each : (shard + 1) * each] + found[cycles + shard * each : cycles + (shard + 1) * each]
            )
        mine[shard, base : base + 8, :] = stats
    for away in range(1, shards):
        peer = lax.rem(me + away, shards)
        part_hop.append(remote(mine.at[peer], parts.at[me], hop_sems, away, "tm", peer))
        part_hop[-1].start()
    parts[me] = mine[me]
    marks[band] = marks_out[band]
    for copy in part_hop:
        copy.wait_recv()

    bin_total = NT // 2
    share = bin_total // 2
    found, raw, scales = [], [], []
    for row in range(2):
        left, right = parts[2 * row], parts[2 * row + 1]
        mean_l, mean_r = left[base : base + 1], right[base : base + 1]
        row_mean = 0.5 * (mean_l + mean_r)
        gap_l, gap_r = mean_l - row_mean, mean_r - row_mean
        squares = left[base + 1 : base + 2] + right[base + 1 : base + 2]
        spread = (squares + share * (gap_l * gap_l + gap_r * gap_r)) / bin_total
        scales.append(jnp.sqrt(spread + EPSILON))
        raw.append(left[:base] + right[:base] - HARM * row_mean)
        found.append(raw[row] / scales[row])
    highest = jnp.maximum(found[0], found[1])
    level = (found[0] + found[1]) / 2
    odd_rows = lax.broadcasted_iota(jnp.int32, (8, LANES), 0) % 2 == 1
    scale_ref[...] = jnp.where(odd_rows, scales[1], scales[0])
    for column in range(lead):
        block = slice(column * each, (column + 1) * each)
        flat_top[pl.ds(column, each, stride=lead), :] = highest[block]
        flat_level[pl.ds(column, each, stride=lead), :] = level[block]
        for row in range(2):
            harm_ref[pl.ds(2 * column + row, each, stride=2 * lead), :] = raw[row][block]
    sent = jnp.maximum(marks_out[...].reshape(bands * slots, LANES), 0)
    tops_out[...] = windows(flat_top[...], sent).reshape(bands, slots, LANES)
    for away in range(1, bands):
        peer = lax.rem(band + away, bands)
        top_hop.append(remote(tops_out.at[peer], tops.at[band], hop_sems, shards + bands + away, "dm", peer))
        top_hop[-1].start()
    tops[band] = tops_out[band]
    for copy in mark_hop:
        copy.wait_recv()
    wanted = marks[...].reshape(bands * slots, LANES)
    floor = windows(flat_level[...], jnp.maximum(wanted, 0)).reshape(bands, slots, LANES)
    for copy in top_hop:
        copy.wait_recv()
    sift_ref[...] = jnp.where(marks[...] >= 0, tops[...] - floor, 0.0)
    own.wait_send()
    for copy in crossing + forwards + mark_hop + part_hop + top_hop:
        copy.wait_send()


def fast_device(tables, series, cand_start, cand_count):
    first, twists, shift, second = tables
    dm_rows, samples_dev = series.shape
    shards, bands = lax.axis_size("tm"), lax.axis_size("dm")
    inner, res = NT // N1, N1 // 2
    kept = inner // 2
    size = samples_dev // LANES
    cycles = NT // (2 * HARM) // N1
    each, lead = cycles // shards, N1 // LANES
    steps = HARM * (HARM + 1) // 2
    depth = sum((harmonic + 1) // 2 for harmonic in range(1, HARM + 1))
    slots = cand_start.shape[3]
    blocks = lead * each
    width = blocks + 8
    vmem, anywhere = pl.BlockSpec(memory_space=pltpu.VMEM), pl.BlockSpec(memory_space=pl.ANY)
    lined = series.reshape(dm_rows, size, LANES).swapaxes(0, 1).reshape(size * dm_rows, LANES)
    low, wide = jnp.bfloat16, jnp.float32
    harm, scale, sifted = pl.pallas_call(
        search_kernel,
        out_shape=(
            jax.ShapeDtypeStruct((dm_rows * blocks, LANES), wide),
            jax.ShapeDtypeStruct((8, LANES), wide),
            jax.ShapeDtypeStruct((bands, slots, LANES), wide),
        ),
        in_specs=[anywhere, vmem, vmem, anywhere, vmem, vmem, anywhere],
        out_specs=(vmem, vmem, vmem),
        scratch_shapes=[
            pltpu.VMEM((dm_rows * size, LANES), wide),
            pltpu.VMEM((shards, size, LANES), wide),
            pltpu.VMEM((size, LANES), wide),
            pltpu.VMEM((2 * first.shape[3], inner), low),
            pltpu.VMEM(first.shape[:3] + (2 * first.shape[3],), low),
            pltpu.VMEM((2, res, inner), wide),
            pltpu.VMEM(second.shape, low),
            pltpu.VMEM((2 * res, inner), wide),
            pltpu.VMEM((4, 2 * res, inner // 4), low),
            pltpu.VMEM((4, 2 * res, inner // 4), low),
            pltpu.VMEM((res // LANES, kept, LANES), wide),
            pltpu.VMEM((2 * cycles, steps * res), low),
            pltpu.VMEM((2, depth * res, res), low),
            pltpu.VMEM((shards, width, LANES), wide),
            pltpu.VMEM((shards, width, LANES), wide),
            pltpu.VMEM((bands, slots, LANES), jnp.int32),
            pltpu.VMEM((bands, slots, LANES), jnp.int32),
            pltpu.VMEM((bands, slots, LANES), wide),
            pltpu.VMEM((bands, slots, LANES), wide),
            pltpu.VMEM((blocks, LANES), wide),
            pltpu.VMEM((blocks, LANES), wide),
            pltpu.SemaphoreType.DMA((3 + CHUNKS,)),
            pltpu.SemaphoreType.DMA((1 + 2 * CHUNKS,)),
            pltpu.SemaphoreType.DMA((1 + 2 * CHUNKS,)),
            pltpu.SemaphoreType.DMA((shards + 2 * bands,)),
            pltpu.SemaphoreType.DMA((shards + 2 * bands,)),
        ],
        compiler_params=pltpu.CompilerParams(
            collective_id=0, has_side_effects=True, vmem_limit_bytes=VMEM_LIMIT
        ),
    )(
        lined, cand_start[0, 0], cand_count[0], jnp.asarray(first), jnp.asarray(twists), jnp.asarray(shift),
        jnp.asarray(second),
    )
    harm = (harm.reshape(-1, 8, LANES) / scale[None]).reshape(harm.shape)
    harmonic_sum = harm.reshape(blocks, dm_rows, LANES).swapaxes(0, 1).reshape(dm_rows, blocks * LANES)
    return (harmonic_sum, sifted[None, None])


def fits(mesh):
    return mesh.shape["tm"] == 4 and BW == LANES


def solution(mesh):
    if fits(mesh):
        tables = dft_tables(mesh.shape["tm"])

        def body(series, cand_start, cand_count):
            if series.shape[0] != 2:
                return per_device(series, cand_start, cand_count)
            return fast_device(tables, series, cand_start, cand_count)
    else:
        body = per_device
    return jax.shard_map(
        body,
        mesh=mesh,
        in_specs=(
            P(("beam", "dm"), "tm"),
            P(("beam", "tm"), "dm", None, None),
            P(("beam", "tm"), "dm", None),
        ),
        out_specs=(P(("beam", "dm"), "tm"), P(("beam", "tm"), "dm", None, None, None)),
        check_vma=False,
    )
```

```python
import math

import jax
import jax.numpy as jnp
import numpy as np
from jax import lax
from jax.experimental import pallas as pl
from jax.experimental.pallas import tpu as pltpu
from jax.sharding import PartitionSpec as P

NT = 524288
N1 = 512
HARM = 8
BW = 128


EPSILON = 1e-06


def contract(pattern, left, right):
    return jnp.einsum(pattern, left, right, precision=lax.Precision.HIGHEST)


def phase_table(left, right, period):
    turns = left[:, None] * right[None, :] % period
    angle = turns.astype(jnp.float32) * (2.0 * math.pi / period)
    return (jnp.cos(angle), jnp.sin(angle))


def twist(real_part, imag_part, cos_twist, sin_twist):
    return (
        real_part * cos_twist + imag_part * sin_twist,
        imag_part * cos_twist - real_part * sin_twist,
    )


def locate_column(column, per_shard):
    return (column // per_shard, column % per_shard)


def harmonic_tables(column_count, shards, per_shard, harmonics):
    listing = [[[] for harmonic in range(harmonics)] for holder in range(shards)]
    for harmonic in range(1, harmonics + 1):
        for residue in range(column_count):
            product = harmonic * residue
            holder, position = locate_column(product % column_count, per_shard)
            listing[holder][harmonic - 1].append((residue, position, product // column_count))
    slot_width = max((max((len(entries) for entries in group)) for group in listing))
    residue_tab = np.zeros((shards, harmonics, slot_width), np.int32)
    position_tab = np.zeros((shards, harmonics, slot_width), np.int32)
    base_tab = np.zeros((shards, harmonics, slot_width), np.int32)
    valid_tab = np.zeros((shards, harmonics, slot_width), np.float32)
    for holder in range(shards):
        for index in range(harmonics):
            for slot, entry in enumerate(listing[holder][index]):
                residue_tab[holder, index, slot] = entry[0]
                position_tab[holder, index, slot] = entry[1]
                base_tab[holder, index, slot] = entry[2]
                valid_tab[holder, index, slot] = 1.0
    return (residue_tab, position_tab, base_tab, valid_tab)


def per_device(series, cand_start, cand_count):
    dm_rows, samples_dev = series.shape
    shards = lax.axis_size("tm")
    my_index = lax.axis_index("tm")
    inner_len = NT // N1
    kept_bins = inner_len // 2
    per_shard = N1 // shards
    columns = jnp.arange(N1, dtype=jnp.int32)
    coarse_rows = samples_dev // inner_len
    rows_local = series.reshape(dm_rows, coarse_rows, inner_len)
    cos_first, sin_first = phase_table(columns, columns, N1)
    narrow = inner_len // shards
    inner_ids = my_index * narrow + jnp.arange(narrow, dtype=jnp.int32)
    cos_twist, sin_twist = phase_table(inner_ids, columns, NT)
    samples = lax.all_to_all(rows_local, "tm", split_axis=2, concat_axis=1, tiled=True)
    real_part = contract("nab,ar->nbr", samples, cos_first)
    imag_part = -contract("nab,ar->nbr", samples, sin_first)
    twist_re, twist_im = twist(real_part, imag_part, cos_twist, sin_twist)
    cos_second, sin_second = phase_table(
        jnp.arange(inner_len, dtype=jnp.int32), jnp.arange(kept_bins, dtype=jnp.int32), inner_len
    )
    part_re = lax.all_to_all(twist_re, "tm", split_axis=2, concat_axis=1, tiled=True)
    part_im = lax.all_to_all(twist_im, "tm", split_axis=2, concat_axis=1, tiled=True)
    x_re = contract("nbr,bk->nrk", part_re, cos_second) + contract(
        "nbr,bk->nrk", part_im, sin_second
    )
    x_im = contract("nbr,bk->nrk", part_im, cos_second) - contract(
        "nbr,bk->nrk", part_re, sin_second
    )
    power_bins = (x_re * x_re + x_im * x_im) / NT
    bin_total = NT // 2
    row_mean = lax.psum(jnp.sum(power_bins, axis=(1, 2)), "tm") / bin_total
    centered = power_bins - row_mean[:, None, None]
    spread = lax.psum(jnp.sum(centered * centered, axis=(1, 2)), "tm") / bin_total
    scores = centered / jnp.sqrt(spread + EPSILON)[:, None, None]
    score_flat = scores.reshape(dm_rows, per_shard * kept_bins)
    cycles = NT // (2 * HARM) // N1
    residue_tab, position_tab, base_tab, valid_tab = harmonic_tables(N1, shards, per_shard, HARM)
    my_positions = jnp.asarray(position_tab)[my_index]
    my_bases = jnp.asarray(base_tab)[my_index]
    my_valid = jnp.asarray(valid_tab)[my_index]
    cycle_ids = jnp.arange(cycles, dtype=jnp.int32)
    picked_parts = []
    for harmonic in range(1, HARM + 1):
        flat_index = (
            my_positions[harmonic - 1][:, None] * kept_bins
            + my_bases[harmonic - 1][:, None]
            + harmonic * cycle_ids[None, :]
        )
        values = jnp.take(score_flat, flat_index.reshape(-1), axis=1).reshape(dm_rows, -1, cycles)
        picked_parts.append(values * my_valid[harmonic - 1][None, :, None])
    picked = jnp.stack(picked_parts, axis=1)
    my_residues = jnp.asarray(residue_tab)[my_index].reshape(-1)
    spread_values = jnp.swapaxes(picked.reshape(dm_rows, -1, cycles), 1, 2)
    dense = jnp.zeros((dm_rows, cycles, N1), jnp.float32).at[:, :, my_residues].add(spread_values)
    dense = dense.reshape(dm_rows, cycles * N1)
    summed = lax.psum_scatter(dense.T, "tm", scatter_dimension=0, tiled=True)
    harmonic_sum = summed.T
    slot_total = cand_start.shape[3]
    offsets = jnp.arange(BW, dtype=jnp.int32)
    starts = cand_start[0, 0]
    counts = cand_count[0, 0]
    live_slots = jnp.arange(slot_total, dtype=jnp.int32)[None, :] < counts[:, None]
    markers = jnp.where(live_slots, starts, -1).astype(jnp.float32)
    bin_spans = starts[..., None] + offsets
    band_level = jnp.sum(harmonic_sum, axis=0) / dm_rows
    gathered = jnp.take(harmonic_sum, bin_spans, axis=1)
    blocks = jnp.moveaxis(gathered, 0, 2)
    blocks_in = lax.all_to_all(blocks, "dm", split_axis=0, concat_axis=0, tiled=True)
    markers_in = lax.all_to_all(markers, "dm", split_axis=0, concat_axis=0, tiled=True)
    chosen = markers_in.astype(jnp.int32)
    level = jnp.take(band_level, jnp.maximum(chosen, 0)[..., None] + offsets, axis=0)
    sifted = jnp.where(chosen[..., None] >= 0, jnp.max(blocks_in, axis=2) - level, 0.0)
    return (harmonic_sum, sifted[None, None])


MESH = pl.DeviceIdType.MESH
LANES = 128
CHUNKS = 4
VMEM_LIMIT = 60 * 1024 * 1024


def split_pair(value):
    high = value.astype(jnp.bfloat16)
    return high, (value - high.astype(jnp.float32)).astype(jnp.bfloat16)


def host_split(table):
    high = table.astype(jnp.bfloat16)
    low = (table - high.astype(np.float64)).astype(jnp.bfloat16)
    return high, low


def dft_tables(shards):
    inner = NT // N1
    kept = inner // 2
    piece = N1 // shards // CHUNKS
    res = N1 // 2
    ids = np.arange(res)
    first = np.empty((shards // 2, CHUNKS, 2 * res, shards // 2, 2, piece), jnp.bfloat16)
    for shard in range(shards):
        for chunk in range(CHUNKS):
            coarse = (shard * CHUNKS + chunk) * piece + np.arange(piece)
            turn = 2.0 * np.pi * (np.outer(ids, coarse) % N1) / N1
            pair = host_split(np.concatenate([np.cos(turn), -np.sin(turn)], axis=0))
            for part in range(2):
                first[shard // 2, chunk, :, shard % 2, part] = pair[part]
    first = first.reshape(shards // 2, CHUNKS, 2 * res, 2 * shards // 2 * piece)

    def waves(turn):
        return np.stack([np.cos(turn), np.sin(turn)], axis=0).astype(np.float32)

    lanes = np.arange(LANES)
    twists = np.stack(
        [
            waves(2.0 * np.pi * np.outer(ids, lanes) / NT),
            waves(2.0 * np.pi * np.outer(ids, np.full(LANES, LANES)) / NT),
        ],
        axis=0,
    )
    shift = waves(2.0 * np.pi * np.outer(np.full(8, res), lanes) / NT)
    second = np.empty((4, kept, inner // 4), jnp.bfloat16)
    for kind in range(4):
        turn = np.outer(4 * np.arange(kept // 4) + kind, np.arange(inner // 4)) % inner
        turn = 2.0 * np.pi * turn / inner
        cos_pair, sin_pair = host_split(np.cos(turn)), host_split(np.sin(turn))
        second[kind] = np.concatenate([cos_pair[0], sin_pair[0], cos_pair[1], sin_pair[1]], axis=0)
    return first, twists, shift, second


def turned(left, right):
    return left[0] * right[0] - left[1] * right[1], left[0] * right[1] + left[1] * right[0]


def windows(table, start):
    count, blocks = start.shape[0], table.shape[0]
    high = table.astype(jnp.bfloat16)
    rest = table - high.astype(jnp.float32)
    middle = rest.astype(jnp.bfloat16)
    low = (rest - middle.astype(jnp.float32)).astype(jnp.bfloat16)
    block = start // LANES
    ids = lax.broadcasted_iota(jnp.int32, (count, blocks), 1)
    hot = jnp.concatenate(
        [jnp.where(ids == block[:, 0:1], 1.0, 0.0), jnp.where(ids == block[:, 0:1] + 1, 1.0, 0.0)], axis=0
    ).astype(jnp.bfloat16)
    picked = jnp.dot(hot, jnp.concatenate([high, middle, low], axis=1), preferred_element_type=jnp.float32)
    picked = picked[:, 0:LANES] + picked[:, LANES : 2 * LANES] + picked[:, 2 * LANES :]
    place = lax.broadcasted_iota(jnp.int32, (count, LANES), 1) + start % LANES
    index = place % LANES
    return jnp.where(
        place < LANES,
        jnp.take_along_axis(picked[0:count], index, axis=1),
        jnp.take_along_axis(picked[count:], index, axis=1),
    )


def search_kernel(
    x_hbm, start_ref, count_ref, first_hbm, twists_ref, shift_ref, second_hbm, harm_ref, scale_ref, sift_ref,
    x_ref, gathered, outgoing, x_tab, first, twist_tab, second, partial, b_high, b_low, power, picks, select,
    mine, parts, marks_out, marks, tops_out, tops, flat_top, flat_level,
    load_sem, send_sem, recv_sem, hop_send, hop_recv,
):
    me, band = lax.axis_index("tm"), lax.axis_index("dm")
    shards, bands = lax.axis_size("tm"), lax.axis_size("dm")
    core, chip = lax.rem(me, 2), me // 2
    sibling = me + 1 - 2 * core
    across = lax.rem(me + 2, 4)
    size = gathered.shape[1]
    step = size // CHUNKS
    inner = partial.shape[1]
    groups = inner // LANES
    piece_rows = step // groups
    res = partial.shape[0] // 2
    kept = power.shape[1]
    slots = sift_ref.shape[1]

    barrier = pltpu.get_barrier_semaphore()
    for axis, count, here in (("tm", shards, me), ("dm", bands, band)):
        for away in range(1, count):
            peer = lax.rem(here + away, count)
            pl.semaphore_signal(barrier, inc=1, device_id={axis: peer}, device_id_type=MESH)
    arrivals = []
    for piece in range(CHUNKS):
        rows = pl.ds(2 * piece * step, 2 * step)
        arrivals.append(pltpu.make_async_copy(x_hbm.at[rows], x_ref.at[rows], load_sem.at[3 + piece]))
        arrivals[-1].start()
    width = first_hbm.shape[3]
    loads = [
        pltpu.make_async_copy(first_hbm, first.at[:, :, :, pl.ds(0, width)], load_sem.at[0]),
        pltpu.make_async_copy(first_hbm, first.at[:, :, :, pl.ds(width, width)], load_sem.at[1]),
        pltpu.make_async_copy(second_hbm, second, load_sem.at[2]),
    ]
    for load in loads:
        load.start()
    for piece in range(CHUNKS):
        arrivals[piece].wait()
        row_a = x_ref[pl.ds(2 * piece * step, step, stride=2), :]
        row_b = x_ref[pl.ds(2 * piece * step + 1, step, stride=2), :]
        outgoing[piece * step : (piece + 1) * step, :] = jnp.where(chip == 0, row_b, row_a)
        gathered[me, piece * step : (piece + 1) * step, :] = jnp.where(chip == 0, row_a, row_b)
    diagonal_ids = lax.broadcasted_iota(jnp.int32, (slots, slots), 0)
    lane_slots = lax.broadcasted_iota(jnp.int32, (slots, slots), 1)
    for target in range(bands):
        line = jnp.where(
            lane_slots[0:1] < count_ref[0:1, target : target + 1], start_ref[target : target + 1, :], -1
        ).astype(jnp.float32)
        column = jnp.sum(jnp.where(diagonal_ids == lane_slots, line, 0.0), axis=1, keepdims=True)
        marks_out[target] = jnp.broadcast_to(column, (slots, LANES)).astype(jnp.int32)
    pl.semaphore_wait(barrier, shards + bands - 2)

    def remote(src, dst, sems, index, axis, peer):
        return pltpu.make_async_remote_copy(
            src_ref=src, dst_ref=dst, send_sem=sems[0].at[index], recv_sem=sems[1].at[index],
            device_id={axis: peer}, device_id_type=MESH,
        )

    row_sems, hop_sems = (send_sem, recv_sem), (hop_send, hop_recv)
    crossing = []
    for piece in range(CHUNKS):
        rows = pl.ds(piece * step, step)
        crossing.append(remote(outgoing.at[rows], gathered.at[me, rows], row_sems, 1 + piece, "tm", across))
        crossing[-1].start()
    own = remote(gathered.at[me], gathered.at[me], row_sems, 0, "tm", sibling)
    own.start()
    mark_hop, part_hop, top_hop = [], [], []
    for away in range(1, bands):
        peer = lax.rem(band + away, bands)
        mark_hop.append(remote(marks_out.at[peer], marks.at[band], hop_sems, shards + away, "dm", peer))
        mark_hop[-1].start()

    odd_core = core == 1
    shifted = (jnp.where(odd_core, shift_ref[0, 0:1], 1.0), jnp.where(odd_core, shift_ref[1, 0:1], 0.0))
    corner = 2.0 * math.pi * LANES * res / NT
    bent = (jnp.where(odd_core, math.cos(corner), 1.0), jnp.where(odd_core, math.sin(corner), 0.0))
    running = turned((twists_ref[0, 0], twists_ref[0, 1]), shifted)
    advance = turned((twists_ref[1, 0], twists_ref[1, 1]), bent)
    for group in range(groups):
        cols = slice(group * LANES, (group + 1) * LANES)
        twist_tab[0, :, cols], twist_tab[1, :, cols] = running
        if group + 1 < groups:
            running = turned(running, advance)

    for load in loads:
        load.wait()
    parity = lax.broadcasted_iota(jnp.int32, (piece_rows, LANES), 0) % 2
    sign = jnp.where(jnp.logical_and(parity == 1, odd_core), -1.0, 1.0)

    quads = groups // 4

    def place(group):
        spot = group % quads * 4 + group // quads
        return slice(spot * LANES, (spot + 1) * LANES)

    def prepare(side, piece):
        for group in range(groups):
            cols = place(group)
            for half in range(2):
                taken = gathered[2 * side + half, pl.ds(piece * step + group, piece_rows, stride=groups), :]
                pair = split_pair(taken * sign)
                for part in range(2):
                    base = (4 * part + 2 * half) * piece_rows
                    x_tab[base : base + piece_rows, cols] = pair[part]
                    x_tab[base + piece_rows : base + 2 * piece_rows, cols] = pair[part]

    def multiply(side, piece, fresh, spans):
        for block in spans:
            cols = slice(block * 256, (block + 1) * 256)
            term = jnp.dot(first[side, piece], x_tab[:, cols], preferred_element_type=jnp.float32)
            partial[:, cols] = term if fresh else partial[:, cols] + term

    def accumulate(side, piece, fresh):
        prepare(side, piece)
        multiply(side, piece, fresh, range(inner // 256))

    own.wait_recv()
    for piece in range(CHUNKS):
        accumulate(chip, piece, piece == 0)

    lane_ids = lax.broadcasted_iota(jnp.int32, (res, res), 1)
    res_ids = lax.broadcasted_iota(jnp.int32, (res, res), 0) + core * res
    plan = []
    slot = 0
    for harmonic in range(1, HARM + 1):
        depth = (harmonic + 1) // 2
        plan.append((harmonic, depth, slot))
        for tile in range(2):
            target = (lane_ids + tile * res) * harmonic - res_ids
            for index in range(depth):
                cycle = index if tile == 0 else harmonic - depth + index
                hit = jnp.where(target == cycle * N1, 1.0, 0.0)
                select[tile, (slot + index) * res : (slot + index + 1) * res, :] = hit.astype(jnp.bfloat16)
        slot += depth

    forwards = []
    for piece in range(CHUNKS):
        rows = pl.ds(piece * step, step)
        crossing[piece].wait_recv()
        forwards.append(
            remote(gathered.at[across, rows], gathered.at[across, rows], row_sems, 1 + CHUNKS + piece, "tm", sibling)
        )
        forwards[-1].start()
        if piece > 0:
            forwards[piece - 1].wait_recv()
            accumulate(1 - chip, piece - 1, False)
    forwards[-1].wait_recv()
    prepare(1 - chip, CHUNKS - 1)

    quarter = inner // 4

    def twisted(block):
        cols, spot = slice(block * LANES, (block + 1) * LANES), place(block)
        return twist(
            partial[0:res, spot], partial[res : 2 * res, spot], twist_tab[0, :, cols], twist_tab[1, :, cols]
        )

    for block in range(quarter // LANES):
        multiply(1 - chip, CHUNKS - 1, False, range(2 * block, 2 * block + 2))
        four = [twisted(block + turn * (quarter // LANES)) for turn in range(4)]
        even_re, even_im = four[0][0] + four[2][0], four[0][1] + four[2][1]
        odd_re, odd_im = four[1][0] + four[3][0], four[1][1] + four[3][1]
        gap_re, gap_im = four[0][0] - four[2][0], four[0][1] - four[2][1]
        lag_re, lag_im = four[1][0] - four[3][0], four[1][1] - four[3][1]
        cols = slice(block * LANES, (block + 1) * LANES)
        for kind, value in enumerate(
            (
                (even_re + odd_re, even_im + odd_im),
                (gap_re + lag_im, gap_im - lag_re),
                (even_re - odd_re, even_im - odd_im),
                (gap_re - lag_im, gap_im + lag_re),
            )
        ):
            for part in range(2):
                rows = slice(part * res, (part + 1) * res)
                b_high[kind, rows, cols], b_low[kind, rows, cols] = split_pair(value[part])

    def against(table, right):
        return lax.dot_general(table, right, (((1,), (1,)), ((), ())), preferred_element_type=jnp.float32)

    fourth = kept // 4
    total = jnp.zeros((1, 1), jnp.float32)
    for kind in range(4):
        both = against(second[kind], b_high[kind])
        less = against(second[kind, 0 : 2 * fourth], b_low[kind])
        by_cos = both[0:fourth] + both[2 * fourth : 3 * fourth] + less[0:fourth]
        by_sin = both[fourth : 2 * fourth] + both[3 * fourth :] + less[fourth:]
        x_re = by_cos[:, 0:res] + by_sin[:, res:]
        x_im = by_cos[:, res:] - by_sin[:, 0:res]
        bins = (x_re * x_re + x_im * x_im) / NT
        total = total + jnp.sum(jnp.sum(bins, axis=0, keepdims=True), axis=1, keepdims=True)
        for column in range(res // LANES):
            power[column, pl.ds(kind, fourth, stride=4), :] = bins[:, column * LANES : (column + 1) * LANES]

    cycles = NT // (2 * HARM) // N1
    sums = [jnp.zeros((2 * cycles, res), jnp.float32) for tile in range(2)]
    slot = 0
    for harmonic, depth, base in plan:
        for cycle in range(harmonic):
            for column in range(res // LANES):
                high, low = split_pair(power[column, pl.ds(cycle, cycles, stride=harmonic), :])
                cols = slice((slot + cycle) * res + column * LANES, (slot + cycle) * res + (column + 1) * LANES)
                picks[0:cycles, cols] = high
                picks[cycles : 2 * cycles, cols] = low
        for tile in range(2):
            begin = (slot + (0 if tile == 0 else harmonic - depth)) * res
            sums[tile] = sums[tile] + jnp.dot(
                picks[:, begin : begin + depth * res],
                select[tile, base * res : (base + depth) * res, :],
                preferred_element_type=jnp.float32,
            )
        slot += harmonic
    mean = total / (kept * res)
    off = power[...] - mean[None]
    deviation = jnp.sum(jnp.sum(jnp.sum(off * off, axis=0), axis=0, keepdims=True), axis=1, keepdims=True)
    stat_rows = lax.broadcasted_iota(jnp.int32, (8, LANES), 0)
    stats = jnp.where(stat_rows == 0, mean, deviation)
    each, lead = cycles // shards, N1 // LANES
    base = lead * each
    for shard in range(shards):
        for column in range(lead):
            found = sums[column * LANES // res][:, column * LANES % res : column * LANES % res + LANES]
            mine[shard, column * each : (column + 1) * each, :] = (
                found[shard * each : (shard + 1) * each] + found[cycles + shard * each : cycles + (shard + 1) * each]
            )
        mine[shard, base : base + 8, :] = stats
    for away in range(1, shards):
        peer = lax.rem(me + away, shards)
        part_hop.append(remote(mine.at[peer], parts.at[me], hop_sems, away, "tm", peer))
        part_hop[-1].start()
    parts[me] = mine[me]
    marks[band] = marks_out[band]
    for copy in part_hop:
        copy.wait_recv()

    bin_total = NT // 2
    share = bin_total // 2
    found, raw, scales = [], [], []
    for row in range(2):
        left, right = parts[2 * row], parts[2 * row + 1]
        mean_l, mean_r = left[base : base + 1], right[base : base + 1]
        row_mean = 0.5 * (mean_l + mean_r)
        gap_l, gap_r = mean_l - row_mean, mean_r - row_mean
        squares = left[base + 1 : base + 2] + right[base + 1 : base + 2]
        spread = (squares + share * (gap_l * gap_l + gap_r * gap_r)) / bin_total
        scales.append(jnp.sqrt(spread + EPSILON))
        raw.append(left[:base] + right[:base] - HARM * row_mean)
        found.append(raw[row] / scales[row])
    highest = jnp.maximum(found[0], found[1])
    level = (found[0] + found[1]) / 2
    odd_rows = lax.broadcasted_iota(jnp.int32, (8, LANES), 0) % 2 == 1
    scale_ref[...] = jnp.where(odd_rows, scales[1], scales[0])
    for column in range(lead):
        block = slice(column * each, (column + 1) * each)
        flat_top[pl.ds(column, each, stride=lead), :] = highest[block]
    sent = jnp.maximum(marks_out[...].reshape(bands * slots, LANES), 0)
    tops_out[...] = windows(flat_top[...], sent).reshape(bands, slots, LANES)
    for away in range(1, bands):
        peer = lax.rem(band + away, bands)
        top_hop.append(remote(tops_out.at[peer], tops.at[band], hop_sems, shards + bands + away, "dm", peer))
        top_hop[-1].start()
    for column in range(lead):
        block = slice(column * each, (column + 1) * each)
        flat_level[pl.ds(column, each, stride=lead), :] = level[block]
        for row in range(2):
            harm_ref[pl.ds(2 * column + row, each, stride=2 * lead), :] = raw[row][block]
    tops[band] = tops_out[band]
    for copy in mark_hop:
        copy.wait_recv()
    wanted = marks[...].reshape(bands * slots, LANES)
    floor = windows(flat_level[...], jnp.maximum(wanted, 0)).reshape(bands, slots, LANES)
    for copy in top_hop:
        copy.wait_recv()
    sift_ref[...] = jnp.where(marks[...] >= 0, tops[...] - floor, 0.0)
    own.wait_send()
    for copy in crossing + forwards + mark_hop + part_hop + top_hop:
        copy.wait_send()


def finish_kernel(raw_ref, scale_ref, excess_ref, harm_ref, sift_ref):
    scale = scale_ref[...]
    for group in range(raw_ref.shape[0] // 8):
        rows = slice(group * 8, (group + 1) * 8)
        harm_ref[rows, :] = raw_ref[rows, :] / scale
    sift_ref[...] = excess_ref[...]


def fast_device(tables, series, cand_start, cand_count):
    first, twists, shift, second = tables
    dm_rows, samples_dev = series.shape
    shards, bands = lax.axis_size("tm"), lax.axis_size("dm")
    inner, res = NT // N1, N1 // 2
    kept = inner // 2
    size = samples_dev // LANES
    cycles = NT // (2 * HARM) // N1
    each, lead = cycles // shards, N1 // LANES
    steps = HARM * (HARM + 1) // 2
    depth = sum((harmonic + 1) // 2 for harmonic in range(1, HARM + 1))
    slots = cand_start.shape[3]
    blocks = lead * each
    width = blocks + 8
    vmem, anywhere = pl.BlockSpec(memory_space=pltpu.VMEM), pl.BlockSpec(memory_space=pl.ANY)
    lined = series.reshape(dm_rows, size, LANES).swapaxes(0, 1).reshape(size * dm_rows, LANES)
    low, wide = jnp.bfloat16, jnp.float32
    harm, scale, sifted = pl.pallas_call(
        search_kernel,
        out_shape=(
            jax.ShapeDtypeStruct((dm_rows * blocks, LANES), wide),
            jax.ShapeDtypeStruct((8, LANES), wide),
            jax.ShapeDtypeStruct((bands, slots, LANES), wide),
        ),
        in_specs=[anywhere, vmem, vmem, anywhere, vmem, vmem, anywhere],
        out_specs=(vmem, vmem, vmem),
        scratch_shapes=[
            pltpu.VMEM((dm_rows * size, LANES), wide),
            pltpu.VMEM((shards, size, LANES), wide),
            pltpu.VMEM((size, LANES), wide),
            pltpu.VMEM((2 * first.shape[3], inner), low),
            pltpu.VMEM(first.shape[:3] + (2 * first.shape[3],), low),
            pltpu.VMEM((2, res, inner), wide),
            pltpu.VMEM(second.shape, low),
            pltpu.VMEM((2 * res, inner), wide),
            pltpu.VMEM((4, 2 * res, inner // 4), low),
            pltpu.VMEM((4, 2 * res, inner // 4), low),
            pltpu.VMEM((res // LANES, kept, LANES), wide),
            pltpu.VMEM((2 * cycles, steps * res), low),
            pltpu.VMEM((2, depth * res, res), low),
            pltpu.VMEM((shards, width, LANES), wide),
            pltpu.VMEM((shards, width, LANES), wide),
            pltpu.VMEM((bands, slots, LANES), jnp.int32),
            pltpu.VMEM((bands, slots, LANES), jnp.int32),
            pltpu.VMEM((bands, slots, LANES), wide),
            pltpu.VMEM((bands, slots, LANES), wide),
            pltpu.VMEM((blocks, LANES), wide),
            pltpu.VMEM((blocks, LANES), wide),
            pltpu.SemaphoreType.DMA((3 + CHUNKS,)),
            pltpu.SemaphoreType.DMA((1 + 2 * CHUNKS,)),
            pltpu.SemaphoreType.DMA((1 + 2 * CHUNKS,)),
            pltpu.SemaphoreType.DMA((shards + 2 * bands,)),
            pltpu.SemaphoreType.DMA((shards + 2 * bands,)),
        ],
        compiler_params=pltpu.CompilerParams(
            collective_id=0, has_side_effects=True, vmem_limit_bytes=VMEM_LIMIT
        ),
    )(
        lined, cand_start[0, 0], cand_count[0], jnp.asarray(first), jnp.asarray(twists), jnp.asarray(shift),
        jnp.asarray(second),
    )
    harm, sifted = pl.pallas_call(
        finish_kernel,
        out_shape=(
            jax.ShapeDtypeStruct(harm.shape, wide),
            jax.ShapeDtypeStruct(sifted.shape, wide),
        ),
        in_specs=[vmem, vmem, vmem],
        out_specs=(vmem, vmem),
    )(harm, scale, sifted)
    harmonic_sum = harm.reshape(blocks, dm_rows, LANES).swapaxes(0, 1).reshape(dm_rows, blocks * LANES)
    return (harmonic_sum, sifted[None, None])


def fits(mesh):
    return mesh.shape["tm"] == 4 and BW == LANES


def solution(mesh):
    if fits(mesh):
        tables = dft_tables(mesh.shape["tm"])

        def body(series, cand_start, cand_count):
            if series.shape[0] != 2:
                return per_device(series, cand_start, cand_count)
            return fast_device(tables, series, cand_start, cand_count)
    else:
        body = per_device
    return jax.shard_map(
        body,
        mesh=mesh,
        in_specs=(
            P(("beam", "dm"), "tm"),
            P(("beam", "tm"), "dm", None, None),
            P(("beam", "tm"), "dm", None),
        ),
        out_specs=(P(("beam", "dm"), "tm"), P(("beam", "tm"), "dm", None, None, None)),
        check_vma=False,
    )
```
